32 devices in a mesh: dp: 16 (over z, y, x), tensor: 2 (over core).
Axes of the slice: x: 2, y: 2, z: 4, core: 2. Of those that a mesh axis runs over, the one named last changes fastest.
Arguments:
- inputs: bfloat16 [32, 1024, 768], P(('dp', 'tensor')), may hold values from -6 to 6
- segment_ids: int32 [32, 1024], P('dp'), may hold values from 0 to 3, never falling along the last dimension, each value on 1 to 512 neighbouring positions
- cotangent: bfloat16 [32, 1024, 768], P(('dp', 'tensor')), may hold values from -6 to 6
- attn_norm_gain: float32 [768], replicated, may hold values from 0.5 to 1.5
- attn_norm_bias: float32 [768], replicated, may hold values from -1.75 to 1.75
- qkv_weight: bfloat16 [3, 768, 768], P(None, None, 'tensor'), may hold values from -0.21875 to 0.21875
- qkv_bias: float32 [3, 768], P(None, 'tensor'), may hold values from -1.75 to 1.75
- attn_sub_gain: float32 [768], P('tensor'), may hold values from 0.5 to 1.5
- attn_sub_bias: float32 [768], P('tensor'), may hold values from -1.75 to 1.75
- out_weight: bfloat16 [768, 768], P('tensor'), may hold values from -0.21875 to 0.21875
- out_bias: float32 [768], replicated, may hold values from -1.75 to 1.75
- ffn_norm_gain: float32 [768], replicated, may hold values from 0.5 to 1.5
- ffn_norm_bias: float32 [768], replicated, may hold values from -1.75 to 1.75
- up_weight: bfloat16 [768, 3072], P(None, 'tensor'), may hold values from -0.21875 to 0.21875
- up_bias: float32 [3072], P('tensor'), may hold values from -1.75 to 1.75
- ffn_sub_gain: float32 [3072], P('tensor'), may hold values from 0.5 to 1.5
- ffn_sub_bias: float32 [3072], P('tensor'), may hold values from -1.75 to 1.75
- down_weight: bfloat16 [3072, 768], P('tensor'), may hold values from -0.109375 to 0.109375
- down_bias: float32 [768], replicated, may hold values from -1.75 to 1.75
Outputs:
- outputs: bfloat16 [32, 1024, 768], P(('dp', 'tensor'))
- input_grad: float32 [32, 1024, 768], P(('dp', 'tensor'))
- attn_norm_gain_grad: float32 [768], replicated
- attn_norm_bias_grad: float32 [768], replicated
- qkv_weight_grad: float32 [3, 768, 768], P(None, None, 'tensor')
- qkv_bias_grad: float32 [3, 768], P(None, 'tensor')
- attn_sub_gain_grad: float32 [768], P('tensor')
- attn_sub_bias_grad: float32 [768], P('tensor')
- out_weight_grad: float32 [768, 768], P('tensor')
- out_bias_grad: float32 [768], replicated
- ffn_norm_gain_grad: float32 [768], replicated
- ffn_norm_bias_grad: float32 [768], replicated
- up_weight_grad: float32 [768, 3072], P(None, 'tensor')
- up_bias_grad: float32 [3072], P('tensor')
- ffn_sub_gain_grad: float32 [3072], P('tensor')
- ffn_sub_bias_grad: float32 [3072], P('tensor')
- down_weight_grad: float32 [3072, 768], P('tensor')
- down_bias_grad: float32 [768], replicated
The draws below stay inside these ranges and needn't reach their ends.
Inputs may be any that keep to these rules, and one draw needn't show every extreme that they name: `segment_ids`: in each row the ids never fall, so each segment is contiguous; a segment holds 1 to 512 tokens, and some segment holds exactly 512.
All inputs are finite; a program needn't handle non-finite values.
Results may differ from the reference program's by a relative error of at most 0.012.
Values may be sent and summed in bfloat16 or wider, within the bound.
A program may use at most 192 MiB of HBM per device.

```python
import math
import jax
import jax.numpy as jnp
import numpy as np
from jax import lax

D = 768
HEADS = 12
HD = 64
FF = 3072
LEN = 1024
BLOCK = 512
SEGS = 4
SEQS = 32


def block_levels(own_key, shape, shards, low, top_value):
    def one(position, shards_of):
        heights = jax.random.uniform(jax.random.fold_in(jax.random.fold_in(own_key, 6), position), (shards_of,), jnp.float32, low / len(shards), top_value / len(shards))
        return jnp.repeat(jnp.exp(heights), shape[position] // shards_of).reshape((-1,) + (1,) * (len(shape) - position - 1))

    factor_of = one(*shards[0])
    for cut in shards[1:]:
        factor_of = factor_of * one(*cut)
    return factor_of


def length_profile(amount, total, bound, slope):
    portions = [(1 << 20) // math.isqrt(rank ** slope) + 1 for rank in range(2, amount + 1)]
    surplus, given = total - bound - (amount - 1), [1] * (amount - 1)
    while surplus > 0:
        candidates = [i for i in range(amount - 1) if given[i] < bound]
        pool, budget = sum([portions[i] for i in candidates]), surplus
        for i in candidates:
            extra = min(bound - given[i], max(1, budget * portions[i] // pool), surplus)
            given[i] = given[i] + extra
            surplus = surplus - extra
    return np.array([bound] + given)


def ragged(rng, count, total, reach, slope):
    if count == 2:
        one = jax.random.randint(rng, (), max(1, total - reach), min(reach, total - 1) + 1)
        return jnp.stack([one, total - one])
    tallies = jnp.asarray(length_profile(count, total, reach, slope), jnp.int32)
    twos = (count - 1) // 2
    giver, receiver = tallies[1:1 + 2 * twos:2], tallies[2:2 + 2 * twos:2]
    room = jnp.minimum(giver - 1, reach - receiver)
    shifted = jax.random.randint(jax.random.fold_in(rng, 1), (twos,), 0, 1 << 20) % (room + 1)
    tallies = tallies.at[1:1 + 2 * twos:2].set(giver - shifted).at[2:2 + 2 * twos:2].set(receiver + shifted)
    return tallies[jax.random.permutation(jax.random.fold_in(rng, 2), count)]


def gaussian(key, shape, scale, most, split=(), kind=jnp.bfloat16):
    gain = block_levels(key, shape, split, -0.22, 0.18) if split else 1.0
    array = jax.random.normal(key, shape, jnp.float32) * scale * gain
    return jnp.minimum(jnp.maximum(array, -most), most).astype(kind)


def setup_inputs(seed: int = 0) -> dict:
    streams_of = jax.random.split(jax.random.key(seed), 20)
    return {
        "inputs": gaussian(streams_of[0], (SEQS, LEN, D), 1.0, 6.0, ((0, 32),)),
        "segment_ids": jax.vmap(lambda own: jnp.searchsorted(jnp.cumsum(ragged(own, SEGS, LEN, LEN // 2, 0)), jnp.arange(LEN), side="right"))(jax.random.split(streams_of[1], SEQS)).reshape((SEQS, LEN)).astype(jnp.int32),
        "cotangent": gaussian(streams_of[2], (SEQS, LEN, D), 1.0, 6.0, ((0, 32),)),
        "attn_norm_gain": jnp.clip(1.0 + 0.1 * jax.random.normal(streams_of[3], (D,), jnp.float32), 0.5, 1.5),
        "attn_norm_bias": gaussian(streams_of[4], (D,), 0.3, 1.75, (), jnp.float32),
        "qkv_weight": gaussian(streams_of[5], (3, D, D), D ** -0.5, 0.21875, ((2, 2),)),
        "qkv_bias": gaussian(streams_of[6], (3, D), 0.3, 1.75, ((1, 2),), jnp.float32),
        "attn_sub_gain": jnp.clip(1.0 + 0.1 * jax.random.normal(streams_of[7], (D,), jnp.float32), 0.5, 1.5),
        "attn_sub_bias": gaussian(streams_of[8], (D,), 0.3, 1.75, ((0, 2),), jnp.float32),
        "out_weight": gaussian(streams_of[9], (D, D), D ** -0.5, 0.21875, ((0, 2),)),
        "out_bias": gaussian(streams_of[10], (D,), 0.3, 1.75, (), jnp.float32),
        "ffn_norm_gain": jnp.clip(1.0 + 0.1 * jax.random.normal(streams_of[11], (D,), jnp.float32), 0.5, 1.5),
        "ffn_norm_bias": gaussian(streams_of[12], (D,), 0.3, 1.75, (), jnp.float32),
        "up_weight": gaussian(streams_of[13], (D, FF), D ** -0.5, 0.21875, ((1, 2),)),
        "up_bias": gaussian(streams_of[14], (FF,), 0.3, 1.75, ((0, 2),), jnp.float32),
        "ffn_sub_gain": jnp.clip(1.0 + 0.1 * jax.random.normal(streams_of[15], (FF,), jnp.float32), 0.5, 1.5),
        "ffn_sub_bias": gaussian(streams_of[16], (FF,), 0.3, 1.75, ((0, 2),), jnp.float32),
        "down_weight": gaussian(streams_of[17], (FF, D), FF ** -0.5, 0.109375, ((0, 2),)),
        "down_bias": gaussian(streams_of[18], (D,), 0.3, 1.75, (), jnp.float32),
    }


@jax.custom_vjp
def low(v):
    return lax.optimization_barrier(v.astype(jnp.bfloat16)).astype(jnp.float32)

@jax.custom_vjp
def low_back(v):
    return v

def low_keep(v):
    return (low(v), None)

def low_pass(kept, grad):
    return (grad,)

def back_keep(v):
    return (v, None)

def back_low(kept, grad):
    return (low(grad),)
low.defvjp(low_keep, low_pass)
low_back.defvjp(back_keep, back_low)

def matmul(left_side, right_side):
    return jnp.einsum('gld,de->gle', left_side, right_side, precision=lax.Precision.HIGHEST)

def layer_norm(values, norm_gain, norm_bias):
    center = lax.optimization_barrier(jnp.mean(values, axis=-1, keepdims=True))
    spread = lax.optimization_barrier(jnp.mean(values * values, axis=-1, keepdims=True)) - center * center
    return (values - center) * lax.rsqrt(spread + 1e-05) * norm_gain + norm_bias

def positions(segment):
    length = segment.shape[-1]
    row_place = jnp.broadcast_to(jnp.arange(length, dtype=jnp.int32), segment.shape)
    before = jnp.concatenate([segment[..., :1] - 1, segment[..., :-1]], axis=-1)
    starts_at = jnp.where(segment != before, row_place, jnp.zeros_like(row_place))
    return row_place - lax.cummax(starts_at, axis=segment.ndim - 1)

def angles(token_place, head_size):
    half_size = head_size // 2
    frequency = jnp.exp(jnp.arange(half_size).astype(jnp.float32) * (-2.0 * math.log(10000.0) / head_size))
    angle_rows = token_place.astype(jnp.float32)[..., None] * frequency
    return (jnp.cos(angle_rows)[..., None, :], jnp.sin(angle_rows)[..., None, :])

def rotate(values, token_place):
    half_size = values.shape[-1] // 2
    cosine, sine_part = angles(token_place, values.shape[-1])
    first_half = values[..., :half_size]
    second = values[..., half_size:]
    return jnp.concatenate([first_half * cosine - second * sine_part, second * cosine + first_half * sine_part], axis=-1)

def attend(queries, key_rows, value_rows, segment):
    length = queries.shape[0]
    block_count = length // BLOCK
    key_place = jnp.arange(length, dtype=jnp.int32)
    score_scale = HD ** (-0.5)

    def one_block(first_row):
        query_block = lax.dynamic_slice_in_dim(queries, first_row, BLOCK, 0)
        query_place = first_row + jnp.arange(BLOCK, dtype=jnp.int32)
        query_segment = lax.dynamic_slice_in_dim(segment, first_row, BLOCK, 0)
        allowed = (query_segment[:, None] == segment[None, :]) & (query_place[:, None] >= key_place[None, :])
        scores = jnp.einsum('qhd,khd->hqk', query_block, key_rows, precision=lax.Precision.HIGHEST) * score_scale
        scores = low_back(scores)
        scores = jnp.where(allowed[None], scores, -1e+30)
        weights = low(jax.nn.softmax(scores, axis=-1))
        return jnp.einsum('hqk,khd->qhd', weights, value_rows, precision=lax.Precision.HIGHEST)
    starts_all = jnp.arange(block_count, dtype=jnp.int32) * BLOCK
    mixed = lax.map(jax.checkpoint(one_block), starts_all)
    return mixed.reshape(queries.shape)

def forward(params, layer_in, segment):
    attn_gain, attn_bias, qkv_w, qkv_b, sub_gain1, sub_bias1, out_w, out_b, ffn_gain, ffn_bias, up_w, up_b, sub_gain2, sub_bias2, down_w, down_b = params
    group_seqs, length, width = layer_in.shape
    token_place = positions(segment)
    head_shape = (group_seqs, length, HEADS, HD)
    normed_one = low(layer_norm(layer_in, attn_gain, attn_bias))
    pre_query = low_back(matmul(normed_one, qkv_w[0]) + qkv_b[0])
    pre_key = low_back(matmul(normed_one, qkv_w[1]) + qkv_b[1])
    pre_value = low_back(matmul(normed_one, qkv_w[2]) + qkv_b[2])
    queries = low(rotate(pre_query.reshape(head_shape), token_place))
    key_rows = low(rotate(pre_key.reshape(head_shape), token_place))
    value_rows = low(pre_value.reshape(head_shape))
    mixed = jax.vmap(attend)(queries, key_rows, value_rows, segment)
    mixed = low_back(mixed.reshape(group_seqs, length, width))
    sub_one = low(layer_norm(mixed, sub_gain1, sub_bias1))
    branch_one = low_back(matmul(sub_one, out_w) + out_b)
    middle = layer_in + branch_one
    normed_two = low(layer_norm(middle, ffn_gain, ffn_bias))
    hidden = low_back(matmul(normed_two, up_w) + up_b)
    active = jax.nn.gelu(hidden, approximate=False)
    sub_two = low(layer_norm(active, sub_gain2, sub_bias2))
    branch_two = low_back(matmul(sub_two, down_w) + down_b)
    return middle + branch_two

def reference(inputs, segment_ids, cotangent, attn_norm_gain, attn_norm_bias, qkv_weight, qkv_bias, attn_sub_gain, attn_sub_bias, out_weight, out_bias, ffn_norm_gain, ffn_norm_bias, up_weight, up_bias, ffn_sub_gain, ffn_sub_bias, down_weight, down_bias):
    params = (attn_norm_gain.astype(jnp.float32), attn_norm_bias.astype(jnp.float32), qkv_weight.astype(jnp.float32), qkv_bias.astype(jnp.float32), attn_sub_gain.astype(jnp.float32), attn_sub_bias.astype(jnp.float32), out_weight.astype(jnp.float32), out_bias.astype(jnp.float32), ffn_norm_gain.astype(jnp.float32), ffn_norm_bias.astype(jnp.float32), up_weight.astype(jnp.float32), up_bias.astype(jnp.float32), ffn_sub_gain.astype(jnp.float32), ffn_sub_bias.astype(jnp.float32), down_weight.astype(jnp.float32), down_bias.astype(jnp.float32))
    group_count = inputs.shape[0] // 4
    in_groups = inputs.astype(jnp.float32).reshape(group_count, 4, LEN, D)
    seg_groups = segment_ids.reshape(group_count, 4, LEN)
    cot_groups = cotangent.astype(jnp.float32).reshape(group_count, 4, LEN, D)
    zeros_all = jax.tree.map(jnp.zeros_like, params)

    def one_group(running, group_item):
        layer_in, layer_seg, layer_cot = group_item

        def apply_layer(param_set, values):
            return forward(param_set, values, layer_seg)
        result, pull = jax.vjp(apply_layer, params, layer_in)
        param_grads, grad_in = pull(layer_cot)
        return (jax.tree.map(jnp.add, running, param_grads), (result.astype(jnp.bfloat16), grad_in))
    totals, (results, grads_in) = lax.scan(one_group, zeros_all, (in_groups, seg_groups, cot_groups))
    return (results.reshape(inputs.shape), grads_in.reshape(inputs.shape), totals[0], totals[1], totals[2], totals[3], totals[4], totals[5], totals[6], totals[7], totals[8], totals[9], totals[10], totals[11], totals[12], totals[13], totals[14], totals[15])
```

```python
import math

import jax
import jax.numpy as jnp
from jax import lax
from jax.experimental import pallas as pl
from jax.experimental.pallas import tpu as pltpu
from jax.sharding import PartitionSpec as P

HD = 64
PAIR = 2 * HD
TILE = 256
REACH = 512
F32 = jnp.float32
BF16 = jnp.bfloat16
VMEM_BYTES = 60 * 1024 * 1024


def nn(a, b):
    return jnp.dot(a, b, preferred_element_type=F32)


def nt(a, b):
    return lax.dot_general(a, b, (((1,), (1,)), ((), ())), preferred_element_type=F32)


def tn(a, b):
    return lax.dot_general(a, b, (((0,), (0,)), ((), ())), preferred_element_type=F32)


def unit_rows(values):
    center = jnp.mean(values, axis=-1, keepdims=True)
    spread = jnp.mean(values * values, axis=-1, keepdims=True) - center * center
    inv = lax.rsqrt(spread + 1e-05)
    return (values - center) * inv, inv


def norm_back(grad, unit, inv, gain):
    scaled = grad * gain
    return inv * (
        scaled
        - jnp.mean(scaled, axis=-1, keepdims=True)
        - unit * jnp.mean(scaled * unit, axis=-1, keepdims=True)
    )


def swap_halves(values):
    lane = lax.broadcasted_iota(jnp.int32, values.shape, 1)
    return jnp.where(
        (lane & (HD // 2)) == 0,
        pltpu.roll(values, PAIR - HD // 2, axis=1),
        pltpu.roll(values, HD // 2, axis=1),
    )


def add_rows(ref, values):
    total = jnp.sum(values, axis=0, keepdims=True)

    @pl.when(pl.program_id(0) == 0)
    def _():
        ref[...] = total

    @pl.when(pl.program_id(0) != 0)
    def _():
        ref[...] += total


def project_kernel(
    x_ref, gain_ref, bias_ref, own_ref, oth_ref, qb_ref, cos_ref, sin_ref, n_ref, q_ref, k_ref, v_ref
):
    unit, _ = unit_rows(x_ref[...].astype(F32))
    normed = (unit * gain_ref[...] + bias_ref[...]).astype(BF16)
    n_ref[...] = normed
    half = own_ref.shape[2]
    cos = cos_ref[...]
    sin = sin_ref[...]
    for j, out_ref in enumerate((q_ref, k_ref, v_ref)):
        for side, w_ref in enumerate((own_ref, oth_ref)):
            pre = nn(normed, w_ref[j]) + qb_ref[j : j + 1, side * half : (side + 1) * half]
            for c in range(half // PAIR):
                part = pre[:, c * PAIR : (c + 1) * PAIR]
                if j < 2:
                    part = part * cos + swap_halves(part) * sin
                part = part.astype(BF16)
                if j == 0:
                    part = part * jnp.asarray(HD**-0.5, BF16)
                at = side * half + c * PAIR
                out_ref[:, at : at + PAIR] = part


def key_range(i):
    return max(0, i * TILE - REACH), (i + 1) * TILE


def head_masks(rows):
    lane = lax.broadcasted_iota(jnp.int32, (rows, PAIR), 1)
    return lane < HD, lane >= HD


def only(mask, values):
    return jnp.where(mask, values, jnp.zeros_like(values))


def attend_kernel(q_ref, k_ref, v_ref, scol_ref, srow_ref, mix_ref, lse_ref, bias_ref):
    blocks = q_ref.shape[0] // TILE

    @pl.when(pl.program_id(0) == 0)
    def _():
        at = 0
        for i in range(blocks):
            k0, k1 = key_range(i)
            shape = (TILE, k1 - k0)
            qi = lax.broadcasted_iota(jnp.int32, shape, 0) + i * TILE
            ki = lax.broadcasted_iota(jnp.int32, shape, 1) + k0
            keep = (scol_ref[i * TILE : (i + 1) * TILE, :] == srow_ref[:, k0:k1]) & (qi >= ki)
            bias_ref[:, at : at + k1 - k0] = jnp.where(keep, 0.0, -1e30).astype(F32)
            at += k1 - k0

    at = 0
    for i in range(blocks):
        k0, k1 = key_range(i)
        width = k1 - k0
        bias = bias_ref[:, at : at + width]
        at += width
        q = q_ref[i * TILE : (i + 1) * TILE, :]
        keys = k_ref[k0:k1, :]
        values = v_ref[k0:k1, :]
        qm = head_masks(TILE)
        km = head_masks(width)
        mixes = []
        lses = []
        for h in range(2):
            scores = nt(only(qm[h], q), keys) + bias
            peak = jnp.max(scores, axis=-1, keepdims=True)
            e = jnp.exp(scores - peak)
            total = jnp.sum(e, axis=-1, keepdims=True)
            weights = (e * (1.0 / total)).astype(BF16)
            mixes.append(nn(weights, only(km[h], values)))
            lses.append(peak + jnp.log(total))
        mix_ref[i * TILE : (i + 1) * TILE, :] = mixes[0] + mixes[1]
        both = jnp.where(
            qm[0], jnp.broadcast_to(lses[0], (TILE, PAIR)), jnp.broadcast_to(lses[1], (TILE, PAIR))
        )
        flipped = both.T
        lse_ref[0, 0:1, i * TILE : (i + 1) * TILE] = flipped[0:1]
        lse_ref[0, 1:2, i * TILE : (i + 1) * TILE] = flipped[HD : HD + 1]


def attend_back_kernel(
    q_ref, k_ref, v_ref, g_ref, lse_ref, scol_ref, srow_ref, cos_ref, sin_ref,
    dq_ref, dk_ref, dv_ref, bq_ref, bk_ref, bv_ref, bias_ref, ka_ref, va_ref,
):
    blocks = q_ref.shape[0] // TILE

    @pl.when(pl.program_id(0) == 0)
    def _():
        at = 0
        for i in range(blocks):
            k0, k1 = key_range(i)
            shape = (k1 - k0, TILE)
            ki = lax.broadcasted_iota(jnp.int32, shape, 0) + k0
            qi = lax.broadcasted_iota(jnp.int32, shape, 1) + i * TILE
            keep = (scol_ref[k0:k1, :] == srow_ref[:, i * TILE : (i + 1) * TILE]) & (qi >= ki)
            bias_ref[at : at + k1 - k0, :] = jnp.where(keep, 0.0, -1e30).astype(F32)
            at += k1 - k0

    ka_ref[...] = jnp.zeros_like(ka_ref)
    va_ref[...] = jnp.zeros_like(va_ref)

    def turn_back(values, rows):
        return values * cos_ref[rows, :] - swap_halves(values) * sin_ref[rows, :]

    sums_q = jnp.zeros((1, PAIR), F32)
    at = 0
    for i in range(blocks):
        k0, k1 = key_range(i)
        width = k1 - k0
        bias = bias_ref[at : at + width, :]
        at += width
        rows = slice(i * TILE, (i + 1) * TILE)
        q = q_ref[rows, :]
        g = g_ref[rows, :]
        keys = k_ref[k0:k1, :]
        values = v_ref[k0:k1, :]
        qm = head_masks(TILE)
        km = head_masks(width)
        qs, gs, ks, ps, ds = [], [], [], [], []
        for h in range(2):
            qh = only(qm[h], q)
            gh = only(qm[h], g)
            scores = nt(keys, qh) + bias
            p = jnp.exp(scores - lse_ref[0, h : h + 1, rows])
            pull = p * nt(values, gh)
            inner = jnp.sum(pull, axis=0, keepdims=True)
            qs.append(qh)
            gs.append(gh)
            ks.append(only(km[h], keys))
            ps.append(p.astype(BF16))
            ds.append((pull - p * inner).astype(BF16))
        q2 = jnp.concatenate(qs, axis=0)
        g2 = jnp.concatenate(gs, axis=0)
        va_ref[k0:k1, :] += nn(jnp.concatenate(ps, axis=1), g2)
        ka_ref[k0:k1, :] += nn(jnp.concatenate(ds, axis=1), q2)
        dq = tn(jnp.concatenate(ds, axis=0), jnp.concatenate(ks, axis=0)) * (HD**-0.5)
        dq = turn_back(dq, rows).astype(BF16)
        dq_ref[rows, :] = dq
        sums_q += jnp.sum(dq.astype(F32), axis=0, keepdims=True)
    bq_ref[...] = sums_q
    dk = turn_back(ka_ref[...], slice(None)).astype(BF16)
    dk_ref[...] = dk
    bk_ref[...] = jnp.sum(dk.astype(F32), axis=0, keepdims=True)
    dv = va_ref[...].astype(BF16)
    dv_ref[...] = dv
    bv_ref[...] = jnp.sum(dv.astype(F32), axis=0, keepdims=True)


def middle_kernel(
    x_ref, mix_ref, cot_ref, sg_ref, sb_ref, wo0_ref, wo1_ref, ob_ref, ng_ref, nb_ref,
    wu0_ref, wu1_ref, ub_ref, fg_ref, fb_ref, wd0_ref, wd1_ref, db_ref,
    out_ref, dmid_ref, dmidb_ref, dmix_ref, sub1_ref, n2_ref, sub2_ref, dhid_ref,
    gsg_ref, gsb_ref, gob_ref, gng_ref, gnb_ref, gub_ref, gfg_ref, gfb_ref, gdb_ref,
    act_ref, slope_ref,
):
    half = wo0_ref.shape[0]
    fhalf = wd0_ref.shape[0]
    ff = 2 * fhalf
    unit1, inv1 = unit_rows(mix_ref[...])
    sub1 = (unit1 * sg_ref[...] + sb_ref[...]).astype(BF16)
    sub1_ref[...] = sub1
    middle = (
        x_ref[...].astype(F32)
        + (nn(sub1[:, :half], wo0_ref[...]) + nn(sub1[:, half:], wo1_ref[...]))
        + ob_ref[...]
    )
    unit2, inv2 = unit_rows(middle)
    normed2 = (unit2 * ng_ref[...] + nb_ref[...]).astype(BF16)
    n2_ref[...] = normed2
    rows = normed2.shape[0]
    total = jnp.zeros((rows, 1), F32)
    square = jnp.zeros((rows, 1), F32)
    step = 512
    for at in range(0, ff, step):
        w_ref, off = (wu0_ref, at) if at < fhalf else (wu1_ref, at - fhalf)
        hidden = nn(normed2, w_ref[:, off : off + step]) + ub_ref[:, at : at + step]
        gate = 0.5 + 0.5 * lax.erf(hidden * (0.5**0.5))
        active = hidden * gate
        act_ref[:, at : at + step] = active
        slope_ref[:, at : at + step] = gate + hidden * (
            jnp.exp(hidden * hidden * -0.5) * (1.0 / math.sqrt(2.0 * math.pi))
        )
        total += jnp.sum(active, axis=-1, keepdims=True)
        square += jnp.sum(active * active, axis=-1, keepdims=True)
    center3 = total * (1.0 / ff)
    inv3 = lax.rsqrt(square * (1.0 / ff) - center3 * center3 + 1e-05)
    cot = cot_ref[...]
    final = middle + db_ref[...]
    t_sum = jnp.zeros((rows, 1), F32)
    t_unit = jnp.zeros((rows, 1), F32)

    def unit3(at):
        return (act_ref[:, at : at + step] - center3) * inv3

    def back2(at):
        w_ref, off = (wd0_ref, at) if at < fhalf else (wd1_ref, at - fhalf)
        return nt(cot, w_ref[off : off + step, :])

    scaled = []
    for at in range(0, ff, step):
        w_ref, off = (wd0_ref, at) if at < fhalf else (wd1_ref, at - fhalf)
        unit = unit3(at)
        act_ref[:, at : at + step] = unit
        sub2 = (unit * fg_ref[:, at : at + step] + fb_ref[:, at : at + step]).astype(BF16)
        sub2_ref[:, at : at + step] = sub2
        final += nn(sub2, w_ref[off : off + step, :])
        grad = back2(at)
        add_rows(gfg_ref.at[:, at : at + step], grad * unit)
        add_rows(gfb_ref.at[:, at : at + step], grad)
        t = grad * fg_ref[:, at : at + step]
        scaled.append(t)
        t_sum += jnp.sum(t, axis=-1, keepdims=True)
        t_unit += jnp.sum(t * unit, axis=-1, keepdims=True)
    out_ref[...] = final.astype(BF16)
    t_sum = t_sum * (1.0 / ff)
    t_unit = t_unit * (1.0 / ff)
    dn2 = jnp.zeros(middle.shape, F32)
    for n, at in enumerate(range(0, ff, step)):
        w_ref, off = (wu0_ref, at) if at < fhalf else (wu1_ref, at - fhalf)
        dact = inv3 * (scaled[n] - t_sum - act_ref[:, at : at + step] * t_unit)
        dhid = (dact * slope_ref[:, at : at + step]).astype(BF16)
        dhid_ref[:, at : at + step] = dhid
        add_rows(gub_ref.at[:, at : at + step], dhid.astype(F32))
        dn2 += nt(dhid, w_ref[:, off : off + step])
    cotf = cot.astype(F32)
    add_rows(gdb_ref, cotf)
    add_rows(gng_ref, dn2 * unit2)
    add_rows(gnb_ref, dn2)
    dmid = cotf + norm_back(dn2, unit2, inv2, ng_ref[...])
    dmid_ref[...] = dmid
    dmidb = dmid.astype(BF16)
    dmidb_ref[...] = dmidb
    add_rows(gob_ref, dmidb.astype(F32))
    ds1 = jnp.concatenate([nt(dmidb, wo0_ref[...]), nt(dmidb, wo1_ref[...])], axis=1)
    add_rows(gsg_ref, ds1 * unit1)
    add_rows(gsb_ref, ds1)
    dmix_ref[...] = norm_back(ds1, unit1, inv1, sg_ref[...]).astype(BF16)


def finish_kernel(
    x_ref, dmid_ref, dq_ref, dk_ref, dv_ref, gain_ref, own_ref, oth_ref, out_ref, gg_ref, gb_ref
):
    half = own_ref.shape[2]
    dn1 = None
    for j, d_ref in enumerate((dq_ref, dk_ref, dv_ref)):
        d = d_ref[...]
        part = nt(d[:, :half], own_ref[j]) + nt(d[:, half:], oth_ref[j])
        dn1 = part if dn1 is None else dn1 + part
    unit, inv = unit_rows(x_ref[...].astype(F32))
    add_rows(gg_ref, dn1 * unit)
    add_rows(gb_ref, dn1)
    out_ref[...] = dmid_ref[...] + norm_back(dn1, unit, inv, gain_ref[...])


def call(kernel, grid, ins, outs, scratch, flops, name):
    moved = sum(a.size * a.dtype.itemsize for a, _, _ in ins)
    moved += sum(math.prod(s) * jnp.dtype(d).itemsize for s, d, _, _ in outs)
    return pl.pallas_call(
        kernel,
        grid=(grid,),
        in_specs=[pl.BlockSpec(b, m) for _, b, m in ins],
        out_specs=[pl.BlockSpec(b, m) for _, _, b, m in outs],
        out_shape=[jax.ShapeDtypeStruct(s, d) for s, d, _, _ in outs],
        scratch_shapes=scratch,
        compiler_params=pltpu.CompilerParams(
            dimension_semantics=("arbitrary",), vmem_limit_bytes=VMEM_BYTES
        ),
        cost_estimate=pl.CostEstimate(flops=flops, bytes_accessed=moved, transcendentals=0),
        name=name,
    )(*[a for a, _, _ in ins])


def fixed(a):
    return (a, a.shape, lambda i, n=a.ndim: (0,) * n)


def tiled(a, tile):
    return (a, (tile, a.shape[1]), lambda i: (i, 0))


def columns(a):
    return (a, (a.shape[0], PAIR), lambda i: (0, i))


def local(
    inputs, segment_ids, cotangent, attn_norm_gain, attn_norm_bias, qkv_weight, qkv_bias,
    attn_sub_gain, attn_sub_bias, out_weight, out_bias, ffn_norm_gain, ffn_norm_bias,
    up_weight, up_bias, ffn_sub_gain, ffn_sub_bias, down_weight, down_bias,
):
    _, length, width = inputs.shape
    half = qkv_weight.shape[2]
    fhalf = up_weight.shape[1]
    ff = 2 * fhalf
    pairs = width // PAIR
    tiles = length // TILE
    swap = [(0, 1), (1, 0)]

    def trade(a):
        return lax.ppermute(a, "tensor", swap)

    x = inputs[0]
    cot = cotangent[0]
    qkv_other = trade(qkv_weight)
    split = jnp.concatenate(
        [qkv_bias.reshape(-1), attn_sub_gain, attn_sub_bias, up_bias, ffn_sub_gain, ffn_sub_bias]
    )
    split_other = trade(split)
    out_other = trade(out_weight)
    up_other = trade(up_weight)
    down_other = trade(down_weight)

    def joined(start, size):
        return jnp.concatenate([split[start : start + size], split_other[start : start + size]])[None]

    qb = jnp.concatenate(
        [split[: 3 * half].reshape(3, half), split_other[: 3 * half].reshape(3, half)], axis=1
    )
    sg = joined(3 * half, half)
    sb = joined(4 * half, half)
    ub = joined(5 * half, fhalf)
    fg = joined(5 * half + fhalf, fhalf)
    fb = joined(5 * half + 2 * fhalf, fhalf)

    segment = lax.dynamic_slice_in_dim(segment_ids, lax.axis_index("tensor"), 1, 0)[0]
    index = jnp.arange(length, dtype=jnp.int32)
    begins = jnp.concatenate([jnp.ones((1,), jnp.bool_), segment[1:] != segment[:-1]])
    place = index - lax.cummax(jnp.where(begins, index, 0))
    frequency = jnp.exp(
        jnp.arange(HD // 2).astype(F32) * (-2.0 * math.log(10000.0) / HD)
    )
    angle = place.astype(F32)[:, None] * frequency
    cosine, sine = jnp.cos(angle), jnp.sin(angle)
    cos = jnp.concatenate([cosine] * 4, axis=1)
    sin = jnp.concatenate([-sine, sine, -sine, sine], axis=1)
    scol = segment[:, None]
    srow = segment[None, :]

    row = lambda v: v[None]
    mm = 2 * length * width
    normed1, q, k, v = call(
        project_kernel,
        tiles,
        [tiled(x, TILE), fixed(row(attn_norm_gain)), fixed(row(attn_norm_bias)), fixed(qkv_weight),
         fixed(qkv_other), fixed(qb), tiled(cos, TILE), tiled(sin, TILE)],
        [((length, width), BF16, (TILE, width), lambda i: (i, 0))] * 4,
        [],
        3 * mm * width,
        "project",
    )
    spans = sum(b - a for a, b in map(key_range, range(tiles)))
    pair_out = lambda dtype: ((length, width), dtype, (length, PAIR), lambda i: (0, i))
    mixed, lse = call(
        attend_kernel,
        pairs,
        [columns(q), columns(k), columns(v), fixed(scol), fixed(srow)],
        [pair_out(F32), ((pairs, 8, length), F32, (1, 8, length), lambda i: (i, 0, 0))],
        [pltpu.VMEM((TILE, spans), F32)],
        8 * mm * spans // tiles,
        "attend",
    )
    tile_out = lambda w, dtype: ((length, w), dtype, (TILE, w), lambda i: (i, 0))
    vec_out = lambda w: ((1, w), F32, (1, w), lambda i: (0, 0))
    (
        outputs, dmid, dmidb, dmix, sub1, normed2, sub2, dhid,
        g_sg, g_sb, g_ob, g_ng, g_nb, g_ub, g_fg, g_fb, g_db,
    ) = call(
        middle_kernel,
        tiles,
        [tiled(x, TILE), tiled(mixed, TILE), tiled(cot, TILE), fixed(sg), fixed(sb), fixed(out_weight),
         fixed(out_other), fixed(row(out_bias)), fixed(row(ffn_norm_gain)), fixed(row(ffn_norm_bias)),
         fixed(up_weight), fixed(up_other), fixed(ub), fixed(fg), fixed(fb), fixed(down_weight),
         fixed(down_other), fixed(row(down_bias))],
        [tile_out(width, BF16), tile_out(width, F32), tile_out(width, BF16), tile_out(width, BF16),
         tile_out(width, BF16), tile_out(width, BF16), tile_out(ff, BF16), tile_out(ff, BF16),
         vec_out(width), vec_out(width), vec_out(width), vec_out(width), vec_out(width),
         vec_out(ff), vec_out(ff), vec_out(ff), vec_out(width)],
        [pltpu.VMEM((TILE, ff), F32), pltpu.VMEM((TILE, ff), F32)],
        2 * mm * (width + 2 * ff),
        "middle",
    )

    def both(left, right, left_side, axis):
        size = (left if left_side else right).shape[1] // 2

        def product(start):
            a = left[:, start : start + size] if left_side else left
            b = right if left_side else right[:, start : start + size]
            return tn(a, b)

        return (product(0) + trade(product(size).astype(BF16)).astype(F32)).astype(BF16)

    down_grad = both(sub2, cot, True, 0)
    up_grad = both(normed2, dhid, False, 1)
    out_grad = both(sub1, dmidb, True, 0)
    down_grad, up_grad, out_grad = lax.psum((down_grad, up_grad, out_grad), "dp")

    dq, dk, dv, g_bq, g_bk, g_bv = call(
        attend_back_kernel,
        pairs,
        [columns(q), columns(k), columns(v), columns(dmix),
         (lse, (1, 8, length), lambda i: (i, 0, 0)), fixed(scol), fixed(srow), fixed(cos), fixed(sin)],
        [pair_out(BF16)] * 3 + [((1, width), F32, (1, PAIR), lambda i: (0, i))] * 3,
        [pltpu.VMEM((spans, TILE), F32), pltpu.VMEM((length, PAIR), F32),
         pltpu.VMEM((length, PAIR), F32)],
        20 * mm * spans // tiles,
        "attend_back",
    )
    qkv_grad = jnp.stack([both(normed1, d, False, 1) for d in (dq, dk, dv)])
    input_grad, g_ag, g_ab = call(
        finish_kernel,
        tiles,
        [tiled(x, TILE), tiled(dmid, TILE), tiled(dq, TILE), tiled(dk, TILE), tiled(dv, TILE),
         fixed(row(attn_norm_gain)), fixed(qkv_weight), fixed(qkv_other)],
        [tile_out(width, F32), vec_out(width), vec_out(width)],
        [],
        3 * mm * width,
        "finish",
    )
    cut = [g_bq, g_bk, g_bv, g_sg, g_sb, g_ub, g_fg, g_fb]
    shared = [g_ag, g_ab, g_ob, g_ng, g_nb, g_db]
    mine = jnp.concatenate([c[0, : c.shape[1] // 2] for c in cut] + [s[0] for s in shared])
    theirs = jnp.concatenate([c[0, c.shape[1] // 2 :] for c in cut] + [s[0] for s in shared])
    small = mine + trade(theirs)
    rows = -(-small.size // half)
    pad = jnp.zeros((rows * half - small.size,), F32)
    small = jnp.concatenate([small, pad]).reshape(rows, half).astype(BF16)
    last = jnp.concatenate([qkv_grad.reshape(3 * width, half), small])
    last = lax.psum(last, "dp").astype(F32)
    qkv_grad = last[: 3 * width].reshape(3, width, half)
    small = last[3 * width :].reshape(-1)
    pieces = []
    at = 0
    for size in [c.shape[1] // 2 for c in cut] + [s.shape[1] for s in shared]:
        pieces.append(small[at : at + size])
        at += size
    g_bq, g_bk, g_bv, g_sg, g_sb, g_ub, g_fg, g_fb, g_ag, g_ab, g_ob, g_ng, g_nb, g_db = pieces
    return (
        outputs[None], input_grad[None], g_ag, g_ab, qkv_grad, jnp.stack([g_bq, g_bk, g_bv]),
        g_sg, g_sb, out_grad.astype(F32), g_ob, g_ng, g_nb, up_grad.astype(F32), g_ub, g_fg, g_fb,
        down_grad.astype(F32), g_db,
    )


def solution(mesh):
    rows = P(("dp", "tensor"), None, None)
    in_specs = (
        rows, P("dp", None), rows, P(), P(), P(None, None, "tensor"), P(None, "tensor"),
        P("tensor"), P("tensor"), P("tensor", None), P(), P(), P(), P(None, "tensor"),
        P("tensor"), P("tensor"), P("tensor"), P("tensor", None), P(),
    )
    out_specs = (
        rows, rows, P(), P(), P(None, None, "tensor"), P(None, "tensor"), P("tensor"), P("tensor"),
        P("tensor", None), P(), P(), P(), P(None, "tensor"), P("tensor"), P("tensor"), P("tensor"),
        P("tensor", None), P(),
    )
    return jax.shard_map(local, mesh=mesh, in_specs=in_specs, out_specs=out_specs, check_vma=False)
```

```python
import functools
import math

import jax
import jax.numpy as jnp
from jax import lax
from jax.experimental import pallas as pl
from jax.experimental.pallas import tpu as pltpu
from jax.sharding import PartitionSpec as P

HD = 64
PAIR = 2 * HD
TILE = 256
REACH = 512
F32 = jnp.float32
BF16 = jnp.bfloat16
VMEM_BYTES = 60 * 1024 * 1024


def nn(a, b):
    return jnp.dot(a, b, preferred_element_type=F32)


def nt(a, b):
    return lax.dot_general(a, b, (((1,), (1,)), ((), ())), preferred_element_type=F32)


def tn(a, b):
    return lax.dot_general(a, b, (((0,), (0,)), ((), ())), preferred_element_type=F32)


def unit_rows(values):
    center = jnp.mean(values, axis=-1, keepdims=True)
    spread = jnp.mean(values * values, axis=-1, keepdims=True) - center * center
    inv = lax.rsqrt(spread + 1e-05)
    return (values - center) * inv, inv


def norm_back(grad, unit, inv, gain):
    scaled = grad * gain
    return inv * (
        scaled
        - jnp.mean(scaled, axis=-1, keepdims=True)
        - unit * jnp.mean(scaled * unit, axis=-1, keepdims=True)
    )


def swap_halves(values):
    lane = lax.broadcasted_iota(jnp.int32, values.shape, 1)
    return jnp.where(
        (lane & (HD // 2)) == 0,
        pltpu.roll(values, PAIR - HD // 2, axis=1),
        pltpu.roll(values, HD // 2, axis=1),
    )


def add_rows(ref, values):
    total = jnp.sum(values, axis=0, keepdims=True)

    @pl.when(pl.program_id(0) == 0)
    def _():
        ref[...] = total

    @pl.when(pl.program_id(0) != 0)
    def _():
        ref[...] += total


def project_kernel(
    x_ref, gain_ref, bias_ref, own_ref, oth_ref, qb_ref, cos_ref, sin_ref, n_ref, q_ref, k_ref, v_ref
):
    unit, _ = unit_rows(x_ref[...].astype(F32))
    normed = (unit * gain_ref[...] + bias_ref[...]).astype(BF16)
    n_ref[...] = normed
    half = own_ref.shape[2]
    cos = cos_ref[...]
    sin = sin_ref[...]
    for j, out_ref in enumerate((q_ref, k_ref, v_ref)):
        for side, w_ref in enumerate((own_ref, oth_ref)):
            pre = nn(normed, w_ref[j]) + qb_ref[j : j + 1, side * half : (side + 1) * half]
            for c in range(half // PAIR):
                part = pre[:, c * PAIR : (c + 1) * PAIR]
                if j < 2:
                    part = part * cos + swap_halves(part) * sin
                part = part.astype(BF16)
                if j == 0:
                    part = part * jnp.asarray(HD**-0.5, BF16)
                at = side * half + c * PAIR
                out_ref[:, at : at + PAIR] = part


def key_range(i):
    return max(0, i * TILE - REACH), (i + 1) * TILE


def head_masks(rows):
    lane = lax.broadcasted_iota(jnp.int32, (rows, PAIR), 1)
    return lane < HD, lane >= HD


def only(mask, values):
    return jnp.where(mask, values, jnp.zeros_like(values))


def attend_kernel(q_ref, k_ref, v_ref, scol_ref, srow_ref, mix_ref, lse_ref, bias_ref):
    blocks = q_ref.shape[0] // TILE

    @pl.when(pl.program_id(0) == 0)
    def _():
        at = 0
        for i in range(blocks):
            k0, k1 = key_range(i)
            shape = (TILE, k1 - k0)
            qi = lax.broadcasted_iota(jnp.int32, shape, 0) + i * TILE
            ki = lax.broadcasted_iota(jnp.int32, shape, 1) + k0
            keep = (scol_ref[i * TILE : (i + 1) * TILE, :] == srow_ref[:, k0:k1]) & (qi >= ki)
            bias_ref[:, at : at + k1 - k0] = jnp.where(keep, 0.0, -1e30).astype(F32)
            at += k1 - k0

    at = 0
    for i in range(blocks):
        k0, k1 = key_range(i)
        width = k1 - k0
        bias = bias_ref[:, at : at + width]
        at += width
        q = q_ref[i * TILE : (i + 1) * TILE, :]
        keys = k_ref[k0:k1, :]
        values = v_ref[k0:k1, :]
        qm = head_masks(TILE)
        km = head_masks(width)
        mixes = []
        lses = []
        for h in range(2):
            scores = nt(only(qm[h], q), keys) + bias
            peak = jnp.max(scores, axis=-1, keepdims=True)
            e = jnp.exp(scores - peak)
            total = jnp.sum(e, axis=-1, keepdims=True)
            weights = (e * (1.0 / total)).astype(BF16)
            mixes.append(nn(weights, only(km[h], values)))
            lses.append(peak + jnp.log(total))
        mix_ref[i * TILE : (i + 1) * TILE, :] = mixes[0] + mixes[1]
        both = jnp.where(
            qm[0], jnp.broadcast_to(lses[0], (TILE, PAIR)), jnp.broadcast_to(lses[1], (TILE, PAIR))
        )
        flipped = both.T
        lse_ref[0, 0:1, i * TILE : (i + 1) * TILE] = flipped[0:1]
        lse_ref[0, 1:2, i * TILE : (i + 1) * TILE] = flipped[HD : HD + 1]


def attend_back_kernel(
    q_ref, k_ref, v_ref, g_ref, lse_ref, scol_ref, srow_ref, cos_ref, sin_ref,
    dq_ref, dk_ref, dv_ref, bq_ref, bk_ref, bv_ref, bias_ref, ka_ref, va_ref,
):
    blocks = q_ref.shape[0] // TILE

    @pl.when(pl.program_id(0) == 0)
    def _():
        at = 0
        for i in range(blocks):
            k0, k1 = key_range(i)
            shape = (k1 - k0, TILE)
            ki = lax.broadcasted_iota(jnp.int32, shape, 0) + k0
            qi = lax.broadcasted_iota(jnp.int32, shape, 1) + i * TILE
            keep = (scol_ref[k0:k1, :] == srow_ref[:, i * TILE : (i + 1) * TILE]) & (qi >= ki)
            bias_ref[at : at + k1 - k0, :] = jnp.where(keep, 0.0, -1e30).astype(F32)
            at += k1 - k0

    ka_ref[...] = jnp.zeros_like(ka_ref)
    va_ref[...] = jnp.zeros_like(va_ref)

    def turn_back(values, rows):
        return values * cos_ref[rows, :] - swap_halves(values) * sin_ref[rows, :]

    sums_q = jnp.zeros((1, PAIR), F32)
    at = 0
    for i in range(blocks):
        k0, k1 = key_range(i)
        width = k1 - k0
        bias = bias_ref[at : at + width, :]
        at += width
        rows = slice(i * TILE, (i + 1) * TILE)
        q = q_ref[rows, :]
        g = g_ref[rows, :]
        keys = k_ref[k0:k1, :]
        values = v_ref[k0:k1, :]
        qm = head_masks(TILE)
        km = head_masks(width)
        qs, gs, ks, ps, ds = [], [], [], [], []
        for h in range(2):
            qh = only(qm[h], q)
            gh = only(qm[h], g)
            scores = nt(keys, qh) + bias
            p = jnp.exp(scores - lse_ref[0, h : h + 1, rows])
            pull = p * nt(values, gh)
            inner = jnp.sum(pull, axis=0, keepdims=True)
            qs.append(qh)
            gs.append(gh)
            ks.append(only(km[h], keys))
            ps.append(p.astype(BF16))
            ds.append((pull - p * inner).astype(BF16))
        q2 = jnp.concatenate(qs, axis=0)
        g2 = jnp.concatenate(gs, axis=0)
        va_ref[k0:k1, :] += nn(jnp.concatenate(ps, axis=1), g2)
        ka_ref[k0:k1, :] += nn(jnp.concatenate(ds, axis=1), q2)
        dq = tn(jnp.concatenate(ds, axis=0), jnp.concatenate(ks, axis=0)) * (HD**-0.5)
        dq = turn_back(dq, rows).astype(BF16)
        dq_ref[rows, :] = dq
        sums_q += jnp.sum(dq.astype(F32), axis=0, keepdims=True)
    bq_ref[...] = sums_q
    dk = turn_back(ka_ref[...], slice(None)).astype(BF16)
    dk_ref[...] = dk
    bk_ref[...] = jnp.sum(dk.astype(F32), axis=0, keepdims=True)
    dv = va_ref[...].astype(BF16)
    dv_ref[...] = dv
    bv_ref[...] = jnp.sum(dv.astype(F32), axis=0, keepdims=True)


def middle_kernel(
    x_ref, mix_ref, cot_ref, sg_ref, sb_ref, wo0_ref, wo1_ref, ob_ref, ng_ref, nb_ref,
    wu0_ref, wu1_ref, ub_ref, fg_ref, fb_ref, wd0_ref, wd1_ref, db_ref,
    out_ref, dmid_ref, dmidb_ref, dmix_ref, sub1_ref, n2_ref, sub2_ref, dhid_ref,
    gsg_ref, gsb_ref, gob_ref, gng_ref, gnb_ref, gub_ref, gfg_ref, gfb_ref, gdb_ref,
    act_ref, slope_ref,
):
    half = wo0_ref.shape[0]
    fhalf = wd0_ref.shape[0]
    ff = 2 * fhalf
    unit1, inv1 = unit_rows(mix_ref[...])
    sub1 = (unit1 * sg_ref[...] + sb_ref[...]).astype(BF16)
    sub1_ref[...] = sub1
    middle = (
        x_ref[...].astype(F32)
        + (nn(sub1[:, :half], wo0_ref[...]) + nn(sub1[:, half:], wo1_ref[...]))
        + ob_ref[...]
    )
    unit2, inv2 = unit_rows(middle)
    normed2 = (unit2 * ng_ref[...] + nb_ref[...]).astype(BF16)
    n2_ref[...] = normed2
    rows = normed2.shape[0]
    total = jnp.zeros((rows, 1), F32)
    square = jnp.zeros((rows, 1), F32)
    step = 512
    for at in range(0, ff, step):
        w_ref, off = (wu0_ref, at) if at < fhalf else (wu1_ref, at - fhalf)
        hidden = nn(normed2, w_ref[:, off : off + step]) + ub_ref[:, at : at + step]
        gate = 0.5 + 0.5 * lax.erf(hidden * (0.5**0.5))
        active = hidden * gate
        act_ref[:, at : at + step] = active
        slope_ref[:, at : at + step] = gate + hidden * (
            jnp.exp(hidden * hidden * -0.5) * (1.0 / math.sqrt(2.0 * math.pi))
        )
        total += jnp.sum(active, axis=-1, keepdims=True)
        square += jnp.sum(active * active, axis=-1, keepdims=True)
    center3 = total * (1.0 / ff)
    inv3 = lax.rsqrt(square * (1.0 / ff) - center3 * center3 + 1e-05)
    cot = cot_ref[...]
    final = middle + db_ref[...]
    t_sum = jnp.zeros((rows, 1), F32)
    t_unit = jnp.zeros((rows, 1), F32)

    def unit3(at):
        return (act_ref[:, at : at + step] - center3) * inv3

    def back2(at):
        w_ref, off = (wd0_ref, at) if at < fhalf else (wd1_ref, at - fhalf)
        return nt(cot, w_ref[off : off + step, :])

    scaled = []
    for at in range(0, ff, step):
        w_ref, off = (wd0_ref, at) if at < fhalf else (wd1_ref, at - fhalf)
        unit = unit3(at)
        act_ref[:, at : at + step] = unit
        sub2 = (unit * fg_ref[:, at : at + step] + fb_ref[:, at : at + step]).astype(BF16)
        sub2_ref[:, at : at + step] = sub2
        final += nn(sub2, w_ref[off : off + step, :])
        grad = back2(at)
        add_rows(gfg_ref.at[:, at : at + step], grad * unit)
        add_rows(gfb_ref.at[:, at : at + step], grad)
        t = grad * fg_ref[:, at : at + step]
        scaled.append(t)
        t_sum += jnp.sum(t, axis=-1, keepdims=True)
        t_unit += jnp.sum(t * unit, axis=-1, keepdims=True)
    out_ref[...] = final.astype(BF16)
    t_sum = t_sum * (1.0 / ff)
    t_unit = t_unit * (1.0 / ff)
    dn2 = jnp.zeros(middle.shape, F32)
    for n, at in enumerate(range(0, ff, step)):
        w_ref, off = (wu0_ref, at) if at < fhalf else (wu1_ref, at - fhalf)
        dact = inv3 * (scaled[n] - t_sum - act_ref[:, at : at + step] * t_unit)
        dhid = (dact * slope_ref[:, at : at + step]).astype(BF16)
        dhid_ref[:, at : at + step] = dhid
        add_rows(gub_ref.at[:, at : at + step], dhid.astype(F32))
        dn2 += nt(dhid, w_ref[:, off : off + step])
    cotf = cot.astype(F32)
    add_rows(gdb_ref, cotf)
    add_rows(gng_ref, dn2 * unit2)
    add_rows(gnb_ref, dn2)
    dmid = cotf + norm_back(dn2, unit2, inv2, ng_ref[...])
    dmid_ref[...] = dmid
    dmidb = dmid.astype(BF16)
    dmidb_ref[...] = dmidb
    add_rows(gob_ref, dmidb.astype(F32))
    ds1 = jnp.concatenate([nt(dmidb, wo0_ref[...]), nt(dmidb, wo1_ref[...])], axis=1)
    add_rows(gsg_ref, ds1 * unit1)
    add_rows(gsb_ref, ds1)
    dmix_ref[...] = norm_back(ds1, unit1, inv1, sg_ref[...]).astype(BF16)


def finish_kernel(
    x_ref, dmid_ref, dq_ref, dk_ref, dv_ref, eq_ref, ek_ref, ev_ref, gain_ref, own_ref, oth_ref,
    out_ref, gg_ref, gb_ref,
):
    dn1 = None
    for j, (d_ref, e_ref) in enumerate(((dq_ref, eq_ref), (dk_ref, ek_ref), (dv_ref, ev_ref))):
        part = nt(d_ref[...], own_ref[j]) + nt(e_ref[...], oth_ref[j])
        dn1 = part if dn1 is None else dn1 + part
    unit, inv = unit_rows(x_ref[...].astype(F32))
    add_rows(gg_ref, dn1 * unit)
    add_rows(gb_ref, dn1)
    out_ref[...] = dmid_ref[...] + norm_back(dn1, unit, inv, gain_ref[...])


def call(kernel, grid, ins, outs, scratch, flops, name):
    moved = sum(a.size * a.dtype.itemsize for a, _, _ in ins)
    moved += sum(math.prod(s) * jnp.dtype(d).itemsize for s, d, _, _ in outs)
    return pl.pallas_call(
        kernel,
        grid=(grid,),
        in_specs=[pl.BlockSpec(b, m) for _, b, m in ins],
        out_specs=[pl.BlockSpec(b, m) for _, _, b, m in outs],
        out_shape=[jax.ShapeDtypeStruct(s, d) for s, d, _, _ in outs],
        scratch_shapes=scratch,
        compiler_params=pltpu.CompilerParams(
            dimension_semantics=("arbitrary",), vmem_limit_bytes=VMEM_BYTES
        ),
        cost_estimate=pl.CostEstimate(flops=flops, bytes_accessed=moved, transcendentals=0),
        name=name,
    )(*[a for a, _, _ in ins])


def fixed(a):
    return (a, a.shape, lambda i, n=a.ndim: (0,) * n)


def tiled(a, tile):
    return (a, (tile, a.shape[1]), lambda i: (i, 0))


def columns(a):
    return (a, (a.shape[0], PAIR), lambda i: (0, i))


def bit_order(count, stream):
    bits = list(range(count.bit_length() - 1))
    turn = min(3, len(bits))
    return bits[stream % turn : turn] + bits[: stream % turn] + bits[turn:]


def dp_scatter(count):
    def run(a, stream, start=0, stop=None):
        me = lax.axis_index("dp")
        for bit in bit_order(count, stream)[start:stop]:
            size = a.shape[0] // 2
            mine = (me >> bit) & 1
            sent = lax.dynamic_slice_in_dim(a, (1 - mine) * size, size, 0)
            kept = lax.dynamic_slice_in_dim(a, mine * size, size, 0)
            got = lax.ppermute(sent, "dp", [(i, i ^ (1 << bit)) for i in range(count)])
            a = (kept.astype(F32) + got.astype(F32)).astype(a.dtype)
        return a

    return run


def dp_gather(count):
    def run(a, stream):
        me = lax.axis_index("dp")
        for bit in reversed(bit_order(count, stream)):
            mine = ((me >> bit) & 1) == 1
            got = lax.ppermute(a, "dp", [(i, i ^ (1 << bit)) for i in range(count)])
            a = jnp.concatenate([jnp.where(mine, got, a), jnp.where(mine, a, got)])
        return a.astype(F32)

    return run


def local(
    scatter, gather,
    inputs, segment_ids, cotangent, attn_norm_gain, attn_norm_bias, qkv_weight, qkv_bias,
    attn_sub_gain, attn_sub_bias, out_weight, out_bias, ffn_norm_gain, ffn_norm_bias,
    up_weight, up_bias, ffn_sub_gain, ffn_sub_bias, down_weight, down_bias,
):
    _, length, width = inputs.shape
    half = qkv_weight.shape[2]
    fhalf = up_weight.shape[1]
    ff = 2 * fhalf
    pairs = width // PAIR
    tiles = length // TILE
    swap = [(0, 1), (1, 0)]

    def trade(a):
        return lax.ppermute(a, "tensor", swap)

    x = inputs[0]
    cot = cotangent[0]
    qkv_other = trade(qkv_weight)
    split = jnp.concatenate(
        [qkv_bias.reshape(-1), attn_sub_gain, attn_sub_bias, up_bias, ffn_sub_gain, ffn_sub_bias]
    )
    split_other = trade(split)
    qkv_other, split_other, out_weight, up_weight, down_weight = lax.optimization_barrier(
        (qkv_other, split_other, out_weight, up_weight, down_weight)
    )
    out_other = trade(out_weight)
    up_other = trade(up_weight)
    down_other = trade(down_weight)

    def joined(start, size):
        return jnp.concatenate([split[start : start + size], split_other[start : start + size]])[None]

    qb = jnp.concatenate(
        [split[: 3 * half].reshape(3, half), split_other[: 3 * half].reshape(3, half)], axis=1
    )
    sg = joined(3 * half, half)
    sb = joined(4 * half, half)
    ub = joined(5 * half, fhalf)
    fg = joined(5 * half + fhalf, fhalf)
    fb = joined(5 * half + 2 * fhalf, fhalf)

    segment = lax.dynamic_slice_in_dim(segment_ids, lax.axis_index("tensor"), 1, 0)[0]
    index = jnp.arange(length, dtype=jnp.int32)
    begins = jnp.concatenate([jnp.ones((1,), jnp.bool_), segment[1:] != segment[:-1]])
    place = index - lax.cummax(jnp.where(begins, index, 0))
    frequency = jnp.exp(
        jnp.arange(HD // 2).astype(F32) * (-2.0 * math.log(10000.0) / HD)
    )
    angle = place.astype(F32)[:, None] * frequency
    cosine, sine = jnp.cos(angle), jnp.sin(angle)
    cos = jnp.concatenate([cosine] * 4, axis=1)
    sin = jnp.concatenate([-sine, sine, -sine, sine], axis=1)
    scol = segment[:, None]
    srow = segment[None, :]

    row = lambda v: v[None]
    mm = 2 * length * width
    normed1, q, k, v = call(
        project_kernel,
        tiles,
        [tiled(x, TILE), fixed(row(attn_norm_gain)), fixed(row(attn_norm_bias)), fixed(qkv_weight),
         fixed(qkv_other), fixed(qb), tiled(cos, TILE), tiled(sin, TILE)],
        [((length, width), BF16, (TILE, width), lambda i: (i, 0))] * 4,
        [],
        3 * mm * width,
        "project",
    )
    spans = sum(b - a for a, b in map(key_range, range(tiles)))
    pair_out = lambda dtype: ((length, width), dtype, (length, PAIR), lambda i: (0, i))
    mixed, lse = call(
        attend_kernel,
        pairs,
        [columns(q), columns(k), columns(v), fixed(scol), fixed(srow)],
        [pair_out(F32), ((pairs, 8, length), F32, (1, 8, length), lambda i: (i, 0, 0))],
        [pltpu.VMEM((TILE, spans), F32)],
        8 * mm * spans // tiles,
        "attend",
    )
    tile_out = lambda w, dtype: ((length, w), dtype, (TILE, w), lambda i: (i, 0))
    vec_out = lambda w: ((1, w), F32, (1, w), lambda i: (0, 0))
    (
        outputs, dmid, dmidb, dmix, sub1, normed2, sub2, dhid,
        g_sg, g_sb, g_ob, g_ng, g_nb, g_ub, g_fg, g_fb, g_db,
    ) = call(
        middle_kernel,
        tiles,
        [tiled(x, TILE), tiled(mixed, TILE), tiled(cot, TILE), fixed(sg), fixed(sb), fixed(out_weight),
         fixed(out_other), fixed(row(out_bias)), fixed(row(ffn_norm_gain)), fixed(row(ffn_norm_bias)),
         fixed(up_weight), fixed(up_other), fixed(ub), fixed(fg), fixed(fb), fixed(down_weight),
         fixed(down_other), fixed(row(down_bias))],
        [tile_out(width, BF16), tile_out(width, F32), tile_out(width, BF16), tile_out(width, BF16),
         tile_out(width, BF16), tile_out(width, BF16), tile_out(ff, BF16), tile_out(ff, BF16),
         vec_out(width), vec_out(width), vec_out(width), vec_out(width), vec_out(width),
         vec_out(ff), vec_out(ff), vec_out(ff), vec_out(width)],
        [pltpu.VMEM((TILE, ff), F32), pltpu.VMEM((TILE, ff), F32)],
        2 * mm * (width + 2 * ff),
        "middle",
    )

    def grown(left, right):
        return tn(left, right).astype(BF16)

    def merged(own, other):
        return (own + trade(other).astype(F32)).astype(BF16)

    down_other_grad = grown(sub2[:, fhalf:], cot)
    up_other_grad = grown(normed2, dhid[:, fhalf:])
    out_other_grad = grown(sub1[:, half:], dmidb)
    down_grad = merged(tn(sub2[:, :fhalf], cot), down_other_grad)
    up_grad = merged(tn(normed2, dhid[:, :fhalf]), up_other_grad)
    out_grad = merged(tn(sub1[:, :half], dmidb), out_other_grad)
    cut_down = 3 * fhalf // 4
    cut_up = 2 * width // 3
    tail_up = up_grad[cut_up:]
    rest = jnp.concatenate([down_grad[cut_down:], out_grad, tail_up[:, :width], tail_up[:, width:]])
    first = [down_grad[:cut_down], up_grad[:cut_up], rest]
    dmix, first = lax.optimization_barrier((dmix, first))

    def back(start, dmix):
        count = pairs // 2
        piece = lambda a: (a, (length, PAIR), lambda i: (0, start + i))
        out = lambda dtype: ((length, half), dtype, (length, PAIR), lambda i: (0, i))
        return call(
            attend_back_kernel,
            count,
            [piece(q), piece(k), piece(v), piece(dmix),
             (lse, (1, 8, length), lambda i: (start + i, 0, 0)), fixed(scol), fixed(srow),
             fixed(cos), fixed(sin)],
            [out(BF16)] * 3 + [((1, half), F32, (1, PAIR), lambda i: (0, i))] * 3,
            [pltpu.VMEM((spans, TILE), F32), pltpu.VMEM((length, PAIR), F32),
             pltpu.VMEM((length, PAIR), F32)],
            10 * mm * spans // tiles,
            "attend_back",
        )

    d_other = back(pairs // 2, dmix)
    qkv_other_grad = [grown(normed1, d) for d in d_other[:3]]
    first = [scatter(a, n, 0, 1) for n, a in enumerate(first)]
    dmix, first, qkv_other_grad = lax.optimization_barrier((dmix, first, qkv_other_grad))
    d_own = back(0, dmix)
    qkv_grad = [merged(tn(normed1, d), o) for d, o in zip(d_own[:3], qkv_other_grad)]
    first = [scatter(a, n, 1, 2) for n, a in enumerate(first)]
    dmid, first, qkv_grad = lax.optimization_barrier((dmid, first, qkv_grad))
    second = [scatter(a, n) for n, a in enumerate(qkv_grad)]
    first = [scatter(a, n, 2) for n, a in enumerate(first)]
    input_grad, g_ag, g_ab = call(
        finish_kernel,
        tiles,
        [tiled(x, TILE), tiled(dmid, TILE)] + [tiled(d, TILE) for d in d_own[:3]]
        + [tiled(d, TILE) for d in d_other[:3]]
        + [fixed(row(attn_norm_gain)), fixed(qkv_weight), fixed(qkv_other)],
        [tile_out(width, F32), vec_out(width), vec_out(width)],
        [],
        3 * mm * width,
        "finish",
    )
    cut = [g_sg, g_sb, g_ub, g_fg, g_fb]
    shared = [g_ag, g_ab, g_ob, g_ng, g_nb, g_db]
    mine = [g[0] for g in d_own[3:]] + [c[0, : c.shape[1] // 2] for c in cut]
    theirs = [g[0] for g in d_other[3:]] + [c[0, c.shape[1] // 2 :] for c in cut]
    sizes = [m.size for m in mine] + [s.shape[1] for s in shared]
    small = jnp.concatenate(mine + [s[0] for s in shared])
    small = small + trade(jnp.concatenate(theirs + [s[0] for s in shared]))
    pad = jnp.zeros((-small.size % (128 * 128),), F32)
    small = scatter(jnp.concatenate([small, pad]).reshape(128, -1), 0)

    first = [gather(a, n) for n, a in enumerate(first)]
    second = [gather(a, n) for n, a in enumerate(second)]
    small = gather(small, 0).reshape(-1)
    down_grad = jnp.concatenate([first[0], first[2][: fhalf - cut_down]])
    at = fhalf - cut_down
    out_grad = first[2][at : at + half]
    at += half
    cut_rows = width - cut_up
    up_grad = jnp.concatenate(
        [
            first[1],
            jnp.concatenate([first[2][at : at + cut_rows], first[2][at + cut_rows :]], axis=1),
        ]
    )
    qkv_grad = jnp.stack(second)
    pieces = []
    at = 0
    for size in sizes:
        pieces.append(small[at : at + size])
        at += size
    g_bq, g_bk, g_bv, g_sg, g_sb, g_ub, g_fg, g_fb, g_ag, g_ab, g_ob, g_ng, g_nb, g_db = pieces
    return (
        outputs[None], input_grad[None], g_ag, g_ab, qkv_grad, jnp.stack([g_bq, g_bk, g_bv]),
        g_sg, g_sb, out_grad, g_ob, g_ng, g_nb, up_grad, g_ub, g_fg, g_fb,
        down_grad, g_db,
    )


def solution(mesh):
    rows = P(("dp", "tensor"), None, None)
    in_specs = (
        rows, P("dp", None), rows, P(), P(), P(None, None, "tensor"), P(None, "tensor"),
        P("tensor"), P("tensor"), P("tensor", None), P(), P(), P(), P(None, "tensor"),
        P("tensor"), P("tensor"), P("tensor"), P("tensor", None), P(),
    )
    out_specs = (
        rows, rows, P(), P(), P(None, None, "tensor"), P(None, "tensor"), P("tensor"), P("tensor"),
        P("tensor", None), P(), P(), P(), P(None, "tensor"), P("tensor"), P("tensor"), P("tensor"),
        P("tensor", None), P(),
    )
    count = mesh.shape["dp"]
    body = functools.partial(local, dp_scatter(count), dp_gather(count))
    return jax.shard_map(body, mesh=mesh, in_specs=in_specs, out_specs=out_specs, check_vma=False)
```

```python
import functools
import math

import jax
import jax.numpy as jnp
from jax import lax
from jax.experimental import pallas as pl
from jax.experimental.pallas import tpu as pltpu
from jax.sharding import PartitionSpec as P

HD = 64
PAIR = 2 * HD
TILE = 256
REACH = 512
F32 = jnp.float32
BF16 = jnp.bfloat16
VMEM_BYTES = 60 * 1024 * 1024


def nn(a, b):
    return jnp.dot(a, b, preferred_element_type=F32)


def nt(a, b):
    return lax.dot_general(a, b, (((1,), (1,)), ((), ())), preferred_element_type=F32)


def tn(a, b):
    return lax.dot_general(a, b, (((0,), (0,)), ((), ())), preferred_element_type=F32)


def unit_rows(values):
    center = jnp.mean(values, axis=-1, keepdims=True)
    spread = jnp.mean(values * values, axis=-1, keepdims=True) - center * center
    inv = lax.rsqrt(spread + 1e-05)
    return (values - center) * inv, inv


def norm_back(grad, unit, inv, gain):
    scaled = grad * gain
    return inv * (
        scaled
        - jnp.mean(scaled, axis=-1, keepdims=True)
        - unit * jnp.mean(scaled * unit, axis=-1, keepdims=True)
    )


def swap_halves(values):
    lane = lax.broadcasted_iota(jnp.int32, values.shape, 1)
    return jnp.where(
        (lane & (HD // 2)) == 0,
        pltpu.roll(values, PAIR - HD // 2, axis=1),
        pltpu.roll(values, HD // 2, axis=1),
    )


def add_rows(ref, values):
    total = jnp.sum(values, axis=0, keepdims=True)

    @pl.when(pl.program_id(0) == 0)
    def _():
        ref[...] = total

    @pl.when(pl.program_id(0) != 0)
    def _():
        ref[...] += total


def project_kernel(
    x_ref, gain_ref, bias_ref, own_ref, oth_ref, qb_ref, cos_ref, sin_ref, n_ref, q_ref, k_ref, v_ref
):
    unit, _ = unit_rows(x_ref[...].astype(F32))
    normed = (unit * gain_ref[...] + bias_ref[...]).astype(BF16)
    n_ref[...] = normed
    half = own_ref.shape[2]
    cos = cos_ref[...]
    sin = sin_ref[...]
    for j, out_ref in enumerate((q_ref, k_ref, v_ref)):
        for side, w_ref in enumerate((own_ref, oth_ref)):
            pre = nn(normed, w_ref[j]) + qb_ref[j : j + 1, side * half : (side + 1) * half]
            for c in range(half // PAIR):
                part = pre[:, c * PAIR : (c + 1) * PAIR]
                if j < 2:
                    part = part * cos + swap_halves(part) * sin
                part = part.astype(BF16)
                if j == 0:
                    part = part * jnp.asarray(HD**-0.5, BF16)
                at = side * half + c * PAIR
                out_ref[:, at : at + PAIR] = part


def key_range(i):
    return max(0, i * TILE - REACH), (i + 1) * TILE


def head_masks(rows):
    lane = lax.broadcasted_iota(jnp.int32, (rows, PAIR), 1)
    return lane < HD, lane >= HD


def only(mask, values):
    return jnp.where(mask, values, jnp.zeros_like(values))


def attend_kernel(q_ref, k_ref, v_ref, scol_ref, srow_ref, mix_ref, lse_ref, bias_ref):
    blocks = q_ref.shape[0] // TILE

    @pl.when(pl.program_id(0) == 0)
    def _():
        at = 0
        for i in range(blocks):
            k0, k1 = key_range(i)
            shape = (TILE, k1 - k0)
            qi = lax.broadcasted_iota(jnp.int32, shape, 0) + i * TILE
            ki = lax.broadcasted_iota(jnp.int32, shape, 1) + k0
            keep = (scol_ref[i * TILE : (i + 1) * TILE, :] == srow_ref[:, k0:k1]) & (qi >= ki)
            bias_ref[:, at : at + k1 - k0] = jnp.where(keep, 0.0, -1e30).astype(F32)
            at += k1 - k0

    at = 0
    for i in range(blocks):
        k0, k1 = key_range(i)
        width = k1 - k0
        bias = bias_ref[:, at : at + width]
        at += width
        q = q_ref[i * TILE : (i + 1) * TILE, :]
        keys = k_ref[k0:k1, :]
        values = v_ref[k0:k1, :]
        qm = head_masks(TILE)
        km = head_masks(width)
        mixes = []
        lses = []
        for h in range(2):
            scores = nt(only(qm[h], q), keys) + bias
            peak = jnp.max(scores, axis=-1, keepdims=True)
            e = jnp.exp(scores - peak)
            total = jnp.sum(e, axis=-1, keepdims=True)
            weights = (e * (1.0 / total)).astype(BF16)
            mixes.append(nn(weights, only(km[h], values)))
            lses.append(peak + jnp.log(total))
        mix_ref[i * TILE : (i + 1) * TILE, :] = mixes[0] + mixes[1]
        both = jnp.where(
            qm[0], jnp.broadcast_to(lses[0], (TILE, PAIR)), jnp.broadcast_to(lses[1], (TILE, PAIR))
        )
        flipped = both.T
        lse_ref[0, 0:1, i * TILE : (i + 1) * TILE] = flipped[0:1]
        lse_ref[0, 1:2, i * TILE : (i + 1) * TILE] = flipped[HD : HD + 1]


def attend_back_kernel(
    q_ref, k_ref, v_ref, g_ref, lse_ref, scol_ref, srow_ref, cos_ref, sin_ref,
    dq_ref, dk_ref, dv_ref, bq_ref, bk_ref, bv_ref, bias_ref, ka_ref, va_ref,
):
    blocks = q_ref.shape[0] // TILE

    @pl.when(pl.program_id(0) == 0)
    def _():
        at = 0
        for i in range(blocks):
            k0, k1 = key_range(i)
            shape = (k1 - k0, TILE)
            ki = lax.broadcasted_iota(jnp.int32, shape, 0) + k0
            qi = lax.broadcasted_iota(jnp.int32, shape, 1) + i * TILE
            keep = (scol_ref[k0:k1, :] == srow_ref[:, i * TILE : (i + 1) * TILE]) & (qi >= ki)
            bias_ref[at : at + k1 - k0, :] = jnp.where(keep, 0.0, -1e30).astype(F32)
            at += k1 - k0

    ka_ref[...] = jnp.zeros_like(ka_ref)
    va_ref[...] = jnp.zeros_like(va_ref)

    def turn_back(values, rows):
        return values * cos_ref[rows, :] - swap_halves(values) * sin_ref[rows, :]

    sums_q = jnp.zeros((1, PAIR), F32)
    at = 0
    for i in range(blocks):
        k0, k1 = key_range(i)
        width = k1 - k0
        bias = bias_ref[at : at + width, :]
        at += width
        rows = slice(i * TILE, (i + 1) * TILE)
        q = q_ref[rows, :]
        g = g_ref[rows, :]
        keys = k_ref[k0:k1, :]
        values = v_ref[k0:k1, :]
        qm = head_masks(TILE)
        km = head_masks(width)
        qs, gs, ks, ps, ds = [], [], [], [], []
        for h in range(2):
            qh = only(qm[h], q)
            gh = only(qm[h], g)
            scores = nt(keys, qh) + bias
            p = jnp.exp(scores - lse_ref[0, h : h + 1, rows])
            pull = p * nt(values, gh)
            inner = jnp.sum(pull, axis=0, keepdims=True)
            qs.append(qh)
            gs.append(gh)
            ks.append(only(km[h], keys))
            ps.append(p.astype(BF16))
            ds.append((pull - p * inner).astype(BF16))
        q2 = jnp.concatenate(qs, axis=0)
        g2 = jnp.concatenate(gs, axis=0)
        va_ref[k0:k1, :] += nn(jnp.concatenate(ps, axis=1), g2)
        ka_ref[k0:k1, :] += nn(jnp.concatenate(ds, axis=1), q2)
        dq = tn(jnp.concatenate(ds, axis=0), jnp.concatenate(ks, axis=0)) * (HD**-0.5)
        dq = turn_back(dq, rows).astype(BF16)
        dq_ref[rows, :] = dq
        sums_q += jnp.sum(dq.astype(F32), axis=0, keepdims=True)
    bq_ref[...] = sums_q
    dk = turn_back(ka_ref[...], slice(None)).astype(BF16)
    dk_ref[...] = dk
    bk_ref[...] = jnp.sum(dk.astype(F32), axis=0, keepdims=True)
    dv = va_ref[...].astype(BF16)
    dv_ref[...] = dv
    bv_ref[...] = jnp.sum(dv.astype(F32), axis=0, keepdims=True)


def middle_kernel(
    x_ref, mix_ref, cot_ref, sg_ref, sb_ref, wo0_ref, wo1_ref, ob_ref, ng_ref, nb_ref,
    wu0_ref, wu1_ref, ub_ref, fg_ref, fb_ref, wd0_ref, wd1_ref, db_ref,
    out_ref, dmid_ref, dmidb_ref, dmix_ref, sub1_ref, n2_ref, sub2_ref, dhid_ref,
    gsg_ref, gsb_ref, gob_ref, gng_ref, gnb_ref, gub_ref, gfg_ref, gfb_ref, gdb_ref,
    act_ref, slope_ref,
):
    half = wo0_ref.shape[0]
    fhalf = wd0_ref.shape[0]
    ff = 2 * fhalf
    unit1, inv1 = unit_rows(mix_ref[...])
    sub1 = (unit1 * sg_ref[...] + sb_ref[...]).astype(BF16)
    sub1_ref[...] = sub1
    middle = (
        x_ref[...].astype(F32)
        + (nn(sub1[:, :half], wo0_ref[...]) + nn(sub1[:, half:], wo1_ref[...]))
        + ob_ref[...]
    )
    unit2, inv2 = unit_rows(middle)
    normed2 = (unit2 * ng_ref[...] + nb_ref[...]).astype(BF16)
    n2_ref[...] = normed2
    rows = normed2.shape[0]
    total = jnp.zeros((rows, 1), F32)
    square = jnp.zeros((rows, 1), F32)
    step = 512
    for at in range(0, ff, step):
        w_ref, off = (wu0_ref, at) if at < fhalf else (wu1_ref, at - fhalf)
        hidden = nn(normed2, w_ref[:, off : off + step]) + ub_ref[:, at : at + step]
        gate = 0.5 + 0.5 * lax.erf(hidden * (0.5**0.5))
        active = hidden * gate
        act_ref[:, at : at + step] = active
        slope_ref[:, at : at + step] = gate + hidden * (
            jnp.exp(hidden * hidden * -0.5) * (1.0 / math.sqrt(2.0 * math.pi))
        )
        total += jnp.sum(active, axis=-1, keepdims=True)
        square += jnp.sum(active * active, axis=-1, keepdims=True)
    center3 = total * (1.0 / ff)
    inv3 = lax.rsqrt(square * (1.0 / ff) - center3 * center3 + 1e-05)
    cot = cot_ref[...]
    final = middle + db_ref[...]
    t_sum = jnp.zeros((rows, 1), F32)
    t_unit = jnp.zeros((rows, 1), F32)

    def unit3(at):
        return (act_ref[:, at : at + step] - center3) * inv3

    def back2(at):
        w_ref, off = (wd0_ref, at) if at < fhalf else (wd1_ref, at - fhalf)
        return nt(cot, w_ref[off : off + step, :])

    scaled = []
    for at in range(0, ff, step):
        w_ref, off = (wd0_ref, at) if at < fhalf else (wd1_ref, at - fhalf)
        unit = unit3(at)
        act_ref[:, at : at + step] = unit
        sub2 = (unit * fg_ref[:, at : at + step] + fb_ref[:, at : at + step]).astype(BF16)
        sub2_ref[:, at : at + step] = sub2
        final += nn(sub2, w_ref[off : off + step, :])
        grad = back2(at)
        add_rows(gfg_ref.at[:, at : at + step], grad * unit)
        add_rows(gfb_ref.at[:, at : at + step], grad)
        t = grad * fg_ref[:, at : at + step]
        scaled.append(t)
        t_sum += jnp.sum(t, axis=-1, keepdims=True)
        t_unit += jnp.sum(t * unit, axis=-1, keepdims=True)
    out_ref[...] = final.astype(BF16)
    t_sum = t_sum * (1.0 / ff)
    t_unit = t_unit * (1.0 / ff)
    dn2 = jnp.zeros(middle.shape, F32)
    for n, at in enumerate(range(0, ff, step)):
        w_ref, off = (wu0_ref, at) if at < fhalf else (wu1_ref, at - fhalf)
        dact = inv3 * (scaled[n] - t_sum - act_ref[:, at : at + step] * t_unit)
        dhid = (dact * slope_ref[:, at : at + step]).astype(BF16)
        dhid_ref[:, at : at + step] = dhid
        add_rows(gub_ref.at[:, at : at + step], dhid.astype(F32))
        dn2 += nt(dhid, w_ref[:, off : off + step])
    cotf = cot.astype(F32)
    add_rows(gdb_ref, cotf)
    add_rows(gng_ref, dn2 * unit2)
    add_rows(gnb_ref, dn2)
    dmid = cotf + norm_back(dn2, unit2, inv2, ng_ref[...])
    dmid_ref[...] = dmid
    dmidb = dmid.astype(BF16)
    dmidb_ref[...] = dmidb
    add_rows(gob_ref, dmidb.astype(F32))
    ds1 = jnp.concatenate([nt(dmidb, wo0_ref[...]), nt(dmidb, wo1_ref[...])], axis=1)
    add_rows(gsg_ref, ds1 * unit1)
    add_rows(gsb_ref, ds1)
    dmix_ref[...] = norm_back(ds1, unit1, inv1, sg_ref[...]).astype(BF16)


def finish_kernel(
    x_ref, dmid_ref, dq_ref, dk_ref, dv_ref, gain_ref, own_ref, oth_ref, out_ref, gg_ref, gb_ref
):
    half = own_ref.shape[2]
    dn1 = None
    for j, d_ref in enumerate((dq_ref, dk_ref, dv_ref)):
        d = d_ref[...]
        part = nt(d[:, :half], own_ref[j]) + nt(d[:, half:], oth_ref[j])
        dn1 = part if dn1 is None else dn1 + part
    unit, inv = unit_rows(x_ref[...].astype(F32))
    add_rows(gg_ref, dn1 * unit)
    add_rows(gb_ref, dn1)
    out_ref[...] = dmid_ref[...] + norm_back(dn1, unit, inv, gain_ref[...])


def call(kernel, grid, ins, outs, scratch, flops, name):
    moved = sum(a.size * a.dtype.itemsize for a, _, _ in ins)
    moved += sum(math.prod(s) * jnp.dtype(d).itemsize for s, d, _, _ in outs)
    return pl.pallas_call(
        kernel,
        grid=(grid,),
        in_specs=[pl.BlockSpec(b, m) for _, b, m in ins],
        out_specs=[pl.BlockSpec(b, m) for _, _, b, m in outs],
        out_shape=[jax.ShapeDtypeStruct(s, d) for s, d, _, _ in outs],
        scratch_shapes=scratch,
        compiler_params=pltpu.CompilerParams(
            dimension_semantics=("arbitrary",), vmem_limit_bytes=VMEM_BYTES
        ),
        cost_estimate=pl.CostEstimate(flops=flops, bytes_accessed=moved, transcendentals=0),
        name=name,
    )(*[a for a, _, _ in ins])


def fixed(a):
    return (a, a.shape, lambda i, n=a.ndim: (0,) * n)


def tiled(a, tile):
    return (a, (tile, a.shape[1]), lambda i: (i, 0))


def columns(a):
    return (a, (a.shape[0], PAIR), lambda i: (0, i))


def bit_order(count, stream):
    bits = list(range(count.bit_length() - 1))
    turn = min(3, len(bits))
    return bits[stream % turn : turn] + bits[: stream % turn] + bits[turn:]


def dp_sum_kernel(count, plan, *refs):
    arrays = max(p[0] for p in plan) + 1
    ins = refs[:arrays]
    outs = refs[arrays : 2 * arrays]
    parts = refs[2 * arrays : 3 * arrays]
    send_sem, recv_sem = refs[3 * arrays :]
    levels = count.bit_length() - 1
    me = lax.axis_index("dp")
    bit_of = lambda bit: (me // (1 << bit)) % 2
    peer = lambda bit: me + (1 - 2 * bit_of(bit)) * (1 << bit)
    barrier = pltpu.get_barrier_semaphore()
    for bit in range(levels):
        pl.semaphore_signal(
            barrier, inc=1, device_id={"dp": peer(bit)}, device_id_type=pl.DeviceIdType.MESH
        )
    pl.semaphore_wait(barrier, levels)

    def copy(src, dst, chain, step, bit):
        return pltpu.make_async_remote_copy(
            src_ref=src, dst_ref=dst, send_sem=send_sem.at[chain, step],
            recv_sem=recv_sem.at[chain, step], device_id={"dp": peer(bit)},
            device_id_type=pl.DeviceIdType.MESH,
        )

    size_at = [count >> (s + 1) for s in range(levels)]
    base_at = [count - (count >> s) for s in range(levels)]
    sent = []

    def halve(chain, step):
        a, stream, c0, c1 = plan[chain]
        bit = bit_order(count, stream)[step]
        size = size_at[step]
        away = (1 - bit_of(bit)) * size
        if step == 0:
            src = ins[a].at[pl.ds(away, size), :, c0:c1]
        else:
            src = parts[a].at[pl.ds(base_at[step - 1] + away, size), :, c0:c1]
        dst = parts[a].at[pl.ds(base_at[step], size), :, c0:c1]
        c = copy(src, dst, chain, step, bit)
        c.start()
        sent.append(c)
        return c

    starts = {}

    def double(chain, step):
        a, stream, c0, c1 = plan[chain]
        order = bit_order(count, stream)
        level = levels - 1 - step
        first = sum(bit_of(order[s]) * size_at[s] for s in range(level + 1))
        view = outs[a].at[pl.ds(first, size_at[level]), :, c0:c1]
        c = copy(view, view, chain, levels + step, order[level])
        c.start()
        sent.append(c)
        return c

    chains = range(len(plan))
    flying = {chain: halve(chain, 0) for chain in chains}
    for step in range(levels):
        for chain in chains:
            a, stream, c0, c1 = plan[chain]
            order = bit_order(count, stream)
            flying[chain].wait_recv()
            kept = bit_of(order[step]) * size_at[step]
            base = base_at[step]

            def total(i):
                own = (
                    ins[a][kept + i, :, c0:c1]
                    if step == 0
                    else parts[a][base_at[step - 1] + kept + i, :, c0:c1]
                )
                return (own.astype(F32) + parts[a][base + i, :, c0:c1].astype(F32)).astype(BF16)

            if step < levels - 1:

                def add(i, carry):
                    parts[a][base + i, :, c0:c1] = total(i)
                    return carry

                lax.fori_loop(0, size_at[step], add, 0)
                flying[chain] = halve(chain, step + 1)
            else:
                mine = sum(bit_of(order[s]) * size_at[s] for s in range(levels))
                outs[a][mine, :, c0:c1] = total(0)
                flying[chain] = double(chain, 0)
    for step in range(levels):
        for chain in chains:
            flying[chain].wait_recv()
            if step < levels - 1:
                flying[chain] = double(chain, step + 1)
    for c in sent:
        c.wait_send()


def dp_sum(count, arrays, plan):
    vmem = pl.BlockSpec(memory_space=pltpu.VMEM)
    levels = count.bit_length() - 1
    return pl.pallas_call(
        functools.partial(dp_sum_kernel, count, plan),
        in_specs=[vmem] * len(arrays),
        out_specs=[vmem] * len(arrays),
        out_shape=[jax.ShapeDtypeStruct(a.shape, a.dtype) for a in arrays],
        scratch_shapes=[pltpu.VMEM(a.shape, a.dtype) for a in arrays]
        + [pltpu.SemaphoreType.DMA((len(plan), 2 * levels))] * 2,
        compiler_params=pltpu.CompilerParams(
            collective_id=0, has_side_effects=True, vmem_limit_bytes=VMEM_BYTES
        ),
        name="dp_sum",
    )(*arrays)


def local(
    count,
    inputs, segment_ids, cotangent, attn_norm_gain, attn_norm_bias, qkv_weight, qkv_bias,
    attn_sub_gain, attn_sub_bias, out_weight, out_bias, ffn_norm_gain, ffn_norm_bias,
    up_weight, up_bias, ffn_sub_gain, ffn_sub_bias, down_weight, down_bias,
):
    _, length, width = inputs.shape
    half = qkv_weight.shape[2]
    fhalf = up_weight.shape[1]
    ff = 2 * fhalf
    pairs = width // PAIR
    tiles = length // TILE
    swap = [(0, 1), (1, 0)]

    def trade(a):
        return lax.ppermute(a, "tensor", swap)

    x = inputs[0]
    cot = cotangent[0]
    qkv_other = trade(qkv_weight)
    split = jnp.concatenate(
        [qkv_bias.reshape(-1), attn_sub_gain, attn_sub_bias, up_bias, ffn_sub_gain, ffn_sub_bias]
    )
    split_other = trade(split)
    out_other = trade(out_weight)
    up_other = trade(up_weight)
    down_other = trade(down_weight)

    def joined(start, size):
        return jnp.concatenate([split[start : start + size], split_other[start : start + size]])[None]

    qb = jnp.concatenate(
        [split[: 3 * half].reshape(3, half), split_other[: 3 * half].reshape(3, half)], axis=1
    )
    sg = joined(3 * half, half)
    sb = joined(4 * half, half)
    ub = joined(5 * half, fhalf)
    fg = joined(5 * half + fhalf, fhalf)
    fb = joined(5 * half + 2 * fhalf, fhalf)

    segment = lax.dynamic_slice_in_dim(segment_ids, lax.axis_index("tensor"), 1, 0)[0]
    index = jnp.arange(length, dtype=jnp.int32)
    begins = jnp.concatenate([jnp.ones((1,), jnp.bool_), segment[1:] != segment[:-1]])
    place = index - lax.cummax(jnp.where(begins, index, 0))
    frequency = jnp.exp(
        jnp.arange(HD // 2).astype(F32) * (-2.0 * math.log(10000.0) / HD)
    )
    angle = place.astype(F32)[:, None] * frequency
    cosine, sine = jnp.cos(angle), jnp.sin(angle)
    cos = jnp.concatenate([cosine] * 4, axis=1)
    sin = jnp.concatenate([-sine, sine, -sine, sine], axis=1)
    scol = segment[:, None]
    srow = segment[None, :]

    row = lambda v: v[None]
    mm = 2 * length * width
    normed1, q, k, v = call(
        project_kernel,
        tiles,
        [tiled(x, TILE), fixed(row(attn_norm_gain)), fixed(row(attn_norm_bias)), fixed(qkv_weight),
         fixed(qkv_other), fixed(qb), tiled(cos, TILE), tiled(sin, TILE)],
        [((length, width), BF16, (TILE, width), lambda i: (i, 0))] * 4,
        [],
        3 * mm * width,
        "project",
    )
    spans = sum(b - a for a, b in map(key_range, range(tiles)))
    pair_out = lambda dtype: ((length, width), dtype, (length, PAIR), lambda i: (0, i))
    mixed, lse = call(
        attend_kernel,
        pairs,
        [columns(q), columns(k), columns(v), fixed(scol), fixed(srow)],
        [pair_out(F32), ((pairs, 8, length), F32, (1, 8, length), lambda i: (i, 0, 0))],
        [pltpu.VMEM((TILE, spans), F32)],
        8 * mm * spans // tiles,
        "attend",
    )
    tile_out = lambda w, dtype: ((length, w), dtype, (TILE, w), lambda i: (i, 0))
    vec_out = lambda w: ((1, w), F32, (1, w), lambda i: (0, 0))
    (
        outputs, dmid, dmidb, dmix, sub1, normed2, sub2, dhid,
        g_sg, g_sb, g_ob, g_ng, g_nb, g_ub, g_fg, g_fb, g_db,
    ) = call(
        middle_kernel,
        tiles,
        [tiled(x, TILE), tiled(mixed, TILE), tiled(cot, TILE), fixed(sg), fixed(sb), fixed(out_weight),
         fixed(out_other), fixed(row(out_bias)), fixed(row(ffn_norm_gain)), fixed(row(ffn_norm_bias)),
         fixed(up_weight), fixed(up_other), fixed(ub), fixed(fg), fixed(fb), fixed(down_weight),
         fixed(down_other), fixed(row(down_bias))],
        [tile_out(width, BF16), tile_out(width, F32), tile_out(width, BF16), tile_out(width, BF16),
         tile_out(width, BF16), tile_out(width, BF16), tile_out(ff, BF16), tile_out(ff, BF16),
         vec_out(width), vec_out(width), vec_out(width), vec_out(width), vec_out(width),
         vec_out(ff), vec_out(ff), vec_out(ff), vec_out(width)],
        [pltpu.VMEM((TILE, ff), F32), pltpu.VMEM((TILE, ff), F32)],
        2 * mm * (width + 2 * ff),
        "middle",
    )

    def merged(left, right, left_side):
        size = (left if left_side else right).shape[1] // 2

        def product(start):
            a = left[:, start : start + size] if left_side else left
            b = right if left_side else right[:, start : start + size]
            return tn(a, b)

        return (product(0) + trade(product(size).astype(BF16)).astype(F32)).astype(BF16)

    down_grad = merged(sub2, cot, True)
    up_grad = merged(normed2, dhid, False)
    out_grad = merged(sub1, dmidb, True)
    dq, dk, dv, g_bq, g_bk, g_bv = call(
        attend_back_kernel,
        pairs,
        [columns(q), columns(k), columns(v), columns(dmix),
         (lse, (1, 8, length), lambda i: (i, 0, 0)), fixed(scol), fixed(srow), fixed(cos), fixed(sin)],
        [pair_out(BF16)] * 3 + [((1, width), F32, (1, PAIR), lambda i: (0, i))] * 3,
        [pltpu.VMEM((spans, TILE), F32), pltpu.VMEM((length, PAIR), F32),
         pltpu.VMEM((length, PAIR), F32)],
        20 * mm * spans // tiles,
        "attend_back",
    )
    qkv_grad = [merged(normed1, d, False) for d in (dq, dk, dv)]
    input_grad, g_ag, g_ab = call(
        finish_kernel,
        tiles,
        [tiled(x, TILE), tiled(dmid, TILE), tiled(dq, TILE), tiled(dk, TILE), tiled(dv, TILE),
         fixed(row(attn_norm_gain)), fixed(qkv_weight), fixed(qkv_other)],
        [tile_out(width, F32), vec_out(width), vec_out(width)],
        [],
        3 * mm * width,
        "finish",
    )
    cut = [g_bq, g_bk, g_bv, g_sg, g_sb, g_ub, g_fg, g_fb]
    shared = [g_ag, g_ab, g_ob, g_ng, g_nb, g_db]
    mine = jnp.concatenate([c[0, : c.shape[1] // 2] for c in cut] + [s[0] for s in shared])
    theirs = jnp.concatenate([c[0, c.shape[1] // 2 :] for c in cut] + [s[0] for s in shared])
    small = mine + trade(theirs)
    pad = jnp.zeros((-small.size % (16 * PAIR * count),), F32)
    small = jnp.concatenate([small, pad]).astype(BF16).reshape(count, -1, PAIR)
    out_grad = jnp.concatenate([out_grad[:, :half], out_grad[:, half:]])
    wide = jnp.concatenate(qkv_grad + [out_grad], axis=1)
    blocks = lambda a: a.reshape(count, a.shape[0] // count, a.shape[1])
    plan = []
    for part in range(2):
        for n, c in enumerate((width, 2 * width, 4 * half)):
            plan.append((n, n, part * c // 2, (part + 1) * c // 2))
    plan.append((3, 2, 0, PAIR))
    down_grad, up_grad, wide, small = dp_sum(
        count, [blocks(down_grad), blocks(up_grad), blocks(wide), small], plan
    )
    down_grad = down_grad.reshape(fhalf, width)
    up_grad = up_grad.reshape(width, fhalf)
    wide = wide.reshape(width, 4 * half).astype(F32)
    qkv_grad = jnp.stack([wide[:, j * half : (j + 1) * half] for j in range(3)])
    out_grad = jnp.concatenate([wide[:half, 3 * half :], wide[half:, 3 * half :]], axis=1)
    small = small.reshape(-1).astype(F32)
    pieces = []
    at = 0
    for size in [c.shape[1] // 2 for c in cut] + [s.shape[1] for s in shared]:
        pieces.append(small[at : at + size])
        at += size
    g_bq, g_bk, g_bv, g_sg, g_sb, g_ub, g_fg, g_fb, g_ag, g_ab, g_ob, g_ng, g_nb, g_db = pieces
    return (
        outputs[None], input_grad[None], g_ag, g_ab, qkv_grad, jnp.stack([g_bq, g_bk, g_bv]),
        g_sg, g_sb, out_grad, g_ob, g_ng, g_nb, up_grad.astype(F32), g_ub, g_fg, g_fb,
        down_grad.astype(F32), g_db,
    )


def solution(mesh):
    rows = P(("dp", "tensor"), None, None)
    in_specs = (
        rows, P("dp", None), rows, P(), P(), P(None, None, "tensor"), P(None, "tensor"),
        P("tensor"), P("tensor"), P("tensor", None), P(), P(), P(), P(None, "tensor"),
        P("tensor"), P("tensor"), P("tensor"), P("tensor", None), P(),
    )
    out_specs = (
        rows, rows, P(), P(), P(None, None, "tensor"), P(None, "tensor"), P("tensor"), P("tensor"),
        P("tensor", None), P(), P(), P(), P(None, "tensor"), P("tensor"), P("tensor"), P("tensor"),
        P("tensor", None), P(),
    )
    body = functools.partial(local, mesh.shape["dp"])
    return jax.shard_map(body, mesh=mesh, in_specs=in_specs, out_specs=out_specs, check_vma=False)
```

```python
import functools
import math

import jax
import jax.numpy as jnp
from jax import lax
from jax.experimental import pallas as pl
from jax.experimental.pallas import tpu as pltpu
from jax.sharding import PartitionSpec as P

HD = 64
PAIR = 2 * HD
TILE = 256
REACH = 512
F32 = jnp.float32
BF16 = jnp.bfloat16
VMEM_BYTES = 60 * 1024 * 1024


def nn(a, b):
    return jnp.dot(a, b, preferred_element_type=F32)


def nt(a, b):
    return lax.dot_general(a, b, (((1,), (1,)), ((), ())), preferred_element_type=F32)


def tn(a, b):
    return lax.dot_general(a, b, (((0,), (0,)), ((), ())), preferred_element_type=F32)


def unit_rows(values):
    center = jnp.mean(values, axis=-1, keepdims=True)
    spread = jnp.mean(values * values, axis=-1, keepdims=True) - center * center
    inv = lax.rsqrt(spread + 1e-05)
    return (values - center) * inv, inv


def norm_back(grad, unit, inv, gain):
    scaled = grad * gain
    return inv * (
        scaled
        - jnp.mean(scaled, axis=-1, keepdims=True)
        - unit * jnp.mean(scaled * unit, axis=-1, keepdims=True)
    )


def swap_halves(values):
    lane = lax.broadcasted_iota(jnp.int32, values.shape, 1)
    return jnp.where(
        (lane & (HD // 2)) == 0,
        pltpu.roll(values, PAIR - HD // 2, axis=1),
        pltpu.roll(values, HD // 2, axis=1),
    )


def add_rows(ref, values):
    total = jnp.sum(values, axis=0, keepdims=True)

    @pl.when(pl.program_id(0) == 0)
    def _():
        ref[...] = total

    @pl.when(pl.program_id(0) != 0)
    def _():
        ref[...] += total


def project_kernel(
    x_ref, gain_ref, bias_ref, own_ref, oth_ref, qb_ref, cos_ref, sin_ref, n_ref, q_ref, k_ref, v_ref
):
    unit, _ = unit_rows(x_ref[...].astype(F32))
    normed = (unit * gain_ref[...] + bias_ref[...]).astype(BF16)
    n_ref[...] = normed
    half = own_ref.shape[2]
    cos = cos_ref[...]
    sin = sin_ref[...]
    for j, out_ref in enumerate((q_ref, k_ref, v_ref)):
        for side, w_ref in enumerate((own_ref, oth_ref)):
            pre = nn(normed, w_ref[j]) + qb_ref[j : j + 1, side * half : (side + 1) * half]
            for c in range(half // PAIR):
                part = pre[:, c * PAIR : (c + 1) * PAIR]
                if j < 2:
                    part = part * cos + swap_halves(part) * sin
                part = part.astype(BF16)
                if j == 0:
                    part = part * jnp.asarray(HD**-0.5, BF16)
                at = side * half + c * PAIR
                out_ref[:, at : at + PAIR] = part


def key_range(i):
    return max(0, i * TILE - REACH), (i + 1) * TILE


def head_masks(rows):
    lane = lax.broadcasted_iota(jnp.int32, (rows, PAIR), 1)
    return lane < HD, lane >= HD


def only(mask, values):
    return jnp.where(mask, values, jnp.zeros_like(values))


def attend_kernel(q_ref, k_ref, v_ref, scol_ref, srow_ref, mix_ref, lse_ref, bias_ref):
    blocks = q_ref.shape[0] // TILE

    @pl.when(pl.program_id(0) == 0)
    def _():
        at = 0
        for i in range(blocks):
            k0, k1 = key_range(i)
            shape = (TILE, k1 - k0)
            qi = lax.broadcasted_iota(jnp.int32, shape, 0) + i * TILE
            ki = lax.broadcasted_iota(jnp.int32, shape, 1) + k0
            keep = (scol_ref[i * TILE : (i + 1) * TILE, :] == srow_ref[:, k0:k1]) & (qi >= ki)
            bias_ref[:, at : at + k1 - k0] = jnp.where(keep, 0.0, -1e30).astype(F32)
            at += k1 - k0

    at = 0
    for i in range(blocks):
        k0, k1 = key_range(i)
        width = k1 - k0
        bias = bias_ref[:, at : at + width]
        at += width
        q = q_ref[i * TILE : (i + 1) * TILE, :]
        keys = k_ref[k0:k1, :]
        values = v_ref[k0:k1, :]
        qm = head_masks(TILE)
        km = head_masks(width)
        mixes = []
        lses = []
        for h in range(2):
            scores = nt(only(qm[h], q), keys) + bias
            peak = jnp.max(scores, axis=-1, keepdims=True)
            e = jnp.exp(scores - peak)
            total = jnp.sum(e, axis=-1, keepdims=True)
            mixes.append(nn(e.astype(BF16), only(km[h], values)) * (1.0 / total))
            lses.append(peak + jnp.log(total))
        mix_ref[i * TILE : (i + 1) * TILE, :] = mixes[0] + mixes[1]
        both = jnp.where(
            qm[0], jnp.broadcast_to(lses[0], (TILE, PAIR)), jnp.broadcast_to(lses[1], (TILE, PAIR))
        )
        flipped = both.T
        lse_ref[0, 0:1, i * TILE : (i + 1) * TILE] = flipped[0:1]
        lse_ref[0, 1:2, i * TILE : (i + 1) * TILE] = flipped[HD : HD + 1]


def attend_back_kernel(
    q_ref, k_ref, v_ref, g_ref, lse_ref, scol_ref, srow_ref, cos_ref, sin_ref,
    dq_ref, dk_ref, dv_ref, bq_ref, bk_ref, bv_ref, bias_ref, ka_ref, va_ref,
):
    blocks = q_ref.shape[0] // TILE

    @pl.when(pl.program_id(0) == 0)
    def _():
        at = 0
        for i in range(blocks):
            k0, k1 = key_range(i)
            shape = (k1 - k0, TILE)
            ki = lax.broadcasted_iota(jnp.int32, shape, 0) + k0
            qi = lax.broadcasted_iota(jnp.int32, shape, 1) + i * TILE
            keep = (scol_ref[k0:k1, :] == srow_ref[:, i * TILE : (i + 1) * TILE]) & (qi >= ki)
            bias_ref[at : at + k1 - k0, :] = jnp.where(keep, 0.0, -1e30).astype(F32)
            at += k1 - k0

    ka_ref[...] = jnp.zeros_like(ka_ref)
    va_ref[...] = jnp.zeros_like(va_ref)

    def turn_back(values, rows):
        return values * cos_ref[rows, :] - swap_halves(values) * sin_ref[rows, :]

    sums_q = jnp.zeros((1, PAIR), F32)
    at = 0
    for i in range(blocks):
        k0, k1 = key_range(i)
        width = k1 - k0
        bias = bias_ref[at : at + width, :]
        at += width
        rows = slice(i * TILE, (i + 1) * TILE)
        q = q_ref[rows, :]
        g = g_ref[rows, :]
        keys = k_ref[k0:k1, :]
        values = v_ref[k0:k1, :]
        qm = head_masks(TILE)
        km = head_masks(width)
        qs, gs, ks, ps, ds = [], [], [], [], []
        for h in range(2):
            qh = only(qm[h], q)
            gh = only(qm[h], g)
            scores = nt(keys, qh) + bias
            p = jnp.exp(scores - lse_ref[0, h : h + 1, rows])
            pull = p * nt(values, gh)
            inner = jnp.sum(pull, axis=0, keepdims=True)
            qs.append(qh)
            gs.append(gh)
            ks.append(only(km[h], keys))
            ps.append(p.astype(BF16))
            ds.append((pull - p * inner).astype(BF16))
        q2 = jnp.concatenate(qs, axis=0)
        g2 = jnp.concatenate(gs, axis=0)
        va_ref[k0:k1, :] += nn(jnp.concatenate(ps, axis=1), g2)
        ka_ref[k0:k1, :] += nn(jnp.concatenate(ds, axis=1), q2)
        dq = tn(jnp.concatenate(ds, axis=0), jnp.concatenate(ks, axis=0)) * (HD**-0.5)
        dq = turn_back(dq, rows).astype(BF16)
        dq_ref[rows, :] = dq
        sums_q += jnp.sum(dq.astype(F32), axis=0, keepdims=True)
    bq_ref[...] = sums_q
    dk = turn_back(ka_ref[...], slice(None)).astype(BF16)
    dk_ref[...] = dk
    bk_ref[...] = jnp.sum(dk.astype(F32), axis=0, keepdims=True)
    dv = va_ref[...].astype(BF16)
    dv_ref[...] = dv
    bv_ref[...] = jnp.sum(dv.astype(F32), axis=0, keepdims=True)


def middle_kernel(
    x_ref, mix_ref, cot_ref, sg_ref, sb_ref, wo0_ref, wo1_ref, ob_ref, ng_ref, nb_ref,
    wu0_ref, wu1_ref, ub_ref, fg_ref, fb_ref, wd0_ref, wd1_ref, db_ref,
    out_ref, dmid_ref, dmidb_ref, dmix_ref, sub1_ref, n2_ref, sub2_ref, dhid_ref,
    gsg_ref, gsb_ref, gob_ref, gng_ref, gnb_ref, gub_ref, gfg_ref, gfb_ref, gdb_ref,
    act_ref, slope_ref,
):
    half = wo0_ref.shape[0]
    fhalf = wd0_ref.shape[0]
    ff = 2 * fhalf
    unit1, inv1 = unit_rows(mix_ref[...])
    sub1 = (unit1 * sg_ref[...] + sb_ref[...]).astype(BF16)
    sub1_ref[...] = sub1
    middle = (
        x_ref[...].astype(F32)
        + (nn(sub1[:, :half], wo0_ref[...]) + nn(sub1[:, half:], wo1_ref[...]))
        + ob_ref[...]
    )
    unit2, inv2 = unit_rows(middle)
    normed2 = (unit2 * ng_ref[...] + nb_ref[...]).astype(BF16)
    n2_ref[...] = normed2
    rows = normed2.shape[0]
    total = jnp.zeros((rows, 1), F32)
    square = jnp.zeros((rows, 1), F32)
    step = 512
    for at in range(0, ff, step):
        w_ref, off = (wu0_ref, at) if at < fhalf else (wu1_ref, at - fhalf)
        hidden = nn(normed2, w_ref[:, off : off + step]) + ub_ref[:, at : at + step]
        gate = 0.5 + 0.5 * lax.erf(hidden * (0.5**0.5))
        active = hidden * gate
        act_ref[:, at : at + step] = active
        slope_ref[:, at : at + step] = gate + hidden * (
            jnp.exp(hidden * hidden * -0.5) * (1.0 / math.sqrt(2.0 * math.pi))
        )
        total += jnp.sum(active, axis=-1, keepdims=True)
        square += jnp.sum(active * active, axis=-1, keepdims=True)
    center3 = total * (1.0 / ff)
    inv3 = lax.rsqrt(square * (1.0 / ff) - center3 * center3 + 1e-05)
    cot = cot_ref[...]
    final = middle + db_ref[...]
    t_sum = jnp.zeros((rows, 1), F32)
    t_unit = jnp.zeros((rows, 1), F32)

    def unit3(at):
        return (act_ref[:, at : at + step] - center3) * inv3

    def back2(at):
        w_ref, off = (wd0_ref, at) if at < fhalf else (wd1_ref, at - fhalf)
        return nt(cot, w_ref[off : off + step, :])

    scaled = []
    for at in range(0, ff, step):
        w_ref, off = (wd0_ref, at) if at < fhalf else (wd1_ref, at - fhalf)
        unit = unit3(at)
        act_ref[:, at : at + step] = unit
        sub2 = (unit * fg_ref[:, at : at + step] + fb_ref[:, at : at + step]).astype(BF16)
        sub2_ref[:, at : at + step] = sub2
        final += nn(sub2, w_ref[off : off + step, :])
        grad = back2(at)
        add_rows(gfg_ref.at[:, at : at + step], grad * unit)
        add_rows(gfb_ref.at[:, at : at + step], grad)
        t = grad * fg_ref[:, at : at + step]
        scaled.append(t)
        t_sum += jnp.sum(t, axis=-1, keepdims=True)
        t_unit += jnp.sum(t * unit, axis=-1, keepdims=True)
    out_ref[...] = final.astype(BF16)
    t_sum = t_sum * (1.0 / ff)
    t_unit = t_unit * (1.0 / ff)
    dn2 = jnp.zeros(middle.shape, F32)
    for n, at in enumerate(range(0, ff, step)):
        w_ref, off = (wu0_ref, at) if at < fhalf else (wu1_ref, at - fhalf)
        dact = inv3 * (scaled[n] - t_sum - act_ref[:, at : at + step] * t_unit)
        dhid = (dact * slope_ref[:, at : at + step]).astype(BF16)
        dhid_ref[:, at : at + step] = dhid
        add_rows(gub_ref.at[:, at : at + step], dhid.astype(F32))
        dn2 += nt(dhid, w_ref[:, off : off + step])
    cotf = cot.astype(F32)
    add_rows(gdb_ref, cotf)
    add_rows(gng_ref, dn2 * unit2)
    add_rows(gnb_ref, dn2)
    dmid = cotf + norm_back(dn2, unit2, inv2, ng_ref[...])
    dmid_ref[...] = dmid
    dmidb = dmid.astype(BF16)
    dmidb_ref[...] = dmidb
    add_rows(gob_ref, dmidb.astype(F32))
    ds1 = jnp.concatenate([nt(dmidb, wo0_ref[...]), nt(dmidb, wo1_ref[...])], axis=1)
    add_rows(gsg_ref, ds1 * unit1)
    add_rows(gsb_ref, ds1)
    dmix_ref[...] = norm_back(ds1, unit1, inv1, sg_ref[...]).astype(BF16)


def finish_kernel(
    x_ref, dmid_ref, dq_ref, dk_ref, dv_ref, gain_ref, own_ref, oth_ref, out_ref, gg_ref, gb_ref
):
    half = own_ref.shape[2]
    dn1 = None
    for j, d_ref in enumerate((dq_ref, dk_ref, dv_ref)):
        d = d_ref[...]
        part = nt(d[:, :half], own_ref[j]) + nt(d[:, half:], oth_ref[j])
        dn1 = part if dn1 is None else dn1 + part
    unit, inv = unit_rows(x_ref[...].astype(F32))
    add_rows(gg_ref, dn1 * unit)
    add_rows(gb_ref, dn1)
    out_ref[...] = dmid_ref[...] + norm_back(dn1, unit, inv, gain_ref[...])


def call(kernel, grid, ins, outs, scratch, flops, name):
    moved = sum(a.size * a.dtype.itemsize for a, _, _ in ins)
    moved += sum(math.prod(s) * jnp.dtype(d).itemsize for s, d, _, _ in outs)
    return pl.pallas_call(
        kernel,
        grid=(grid,),
        in_specs=[pl.BlockSpec(b, m) for _, b, m in ins],
        out_specs=[pl.BlockSpec(b, m) for _, _, b, m in outs],
        out_shape=[jax.ShapeDtypeStruct(s, d) for s, d, _, _ in outs],
        scratch_shapes=scratch,
        compiler_params=pltpu.CompilerParams(
            dimension_semantics=("arbitrary",), vmem_limit_bytes=VMEM_BYTES
        ),
        cost_estimate=pl.CostEstimate(flops=flops, bytes_accessed=moved, transcendentals=0),
        name=name,
    )(*[a for a, _, _ in ins])


def fixed(a):
    return (a, a.shape, lambda i, n=a.ndim: (0,) * n)


def tiled(a, tile):
    return (a, (tile, a.shape[1]), lambda i: (i, 0))


def columns(a):
    return (a, (a.shape[0], PAIR), lambda i: (0, i))


def bit_order(count, stream):
    bits = list(range(count.bit_length() - 1))
    turn = min(3, len(bits))
    return bits[stream % turn : turn] + bits[: stream % turn] + bits[turn:]


def dp_sum_kernel(count, plan, *refs):
    arrays = max(p[0] for p in plan) + 1
    ins = refs[:arrays]
    outs = refs[arrays : 2 * arrays]
    parts = refs[2 * arrays : 3 * arrays]
    send_sem, recv_sem = refs[3 * arrays :]
    levels = count.bit_length() - 1
    me = lax.axis_index("dp")
    bit_of = lambda bit: (me // (1 << bit)) % 2
    peer = lambda bit: me + (1 - 2 * bit_of(bit)) * (1 << bit)
    barrier = pltpu.get_barrier_semaphore()
    for bit in range(levels):
        pl.semaphore_signal(
            barrier, inc=1, device_id={"dp": peer(bit)}, device_id_type=pl.DeviceIdType.MESH
        )
    pl.semaphore_wait(barrier, levels)

    def copy(src, dst, chain, step, bit):
        return pltpu.make_async_remote_copy(
            src_ref=src, dst_ref=dst, send_sem=send_sem.at[chain, step],
            recv_sem=recv_sem.at[chain, step], device_id={"dp": peer(bit)},
            device_id_type=pl.DeviceIdType.MESH,
        )

    size_at = [count >> (s + 1) for s in range(levels)]
    base_at = [count - (count >> s) for s in range(levels)]
    sent = []

    def halve(chain, step):
        a, stream, c0, c1 = plan[chain][:4]
        bit = bit_order(count, stream)[step]
        size = size_at[step]
        away = (1 - bit_of(bit)) * size
        if step == 0:
            src = ins[a].at[pl.ds(away, size), :, c0:c1]
        else:
            src = parts[a].at[pl.ds(base_at[step - 1] + away, size), :, c0:c1]
        dst = parts[a].at[pl.ds(base_at[step], size), :, c0:c1]
        c = copy(src, dst, chain, step, bit)
        c.start()
        sent.append(c)
        return c

    starts = {}

    def double(chain, step):
        a, stream, c0, c1 = plan[chain][:4]
        order = bit_order(count, stream)
        level = levels - 1 - step
        first = sum(bit_of(order[s]) * size_at[s] for s in range(level + 1))
        view = outs[a].at[pl.ds(first, size_at[level]), :, c0:c1]
        c = copy(view, view, chain, levels + step, order[level])
        c.start()
        sent.append(c)
        return c

    flying = [halve(chain, 0) for chain in range(len(plan))]

    def advance(chain, step):
        a, stream, c0, c1 = plan[chain][:4]
        flying[chain].wait_recv()
        if step >= levels:
            if step < 2 * levels - 1:
                flying[chain] = double(chain, step - levels + 1)
            return
        order = bit_order(count, stream)
        kept = bit_of(order[step]) * size_at[step]
        base = base_at[step]

        def total(i):
            own = (
                ins[a][kept + i, :, c0:c1]
                if step == 0
                else parts[a][base_at[step - 1] + kept + i, :, c0:c1]
            )
            return (own.astype(F32) + parts[a][base + i, :, c0:c1].astype(F32)).astype(BF16)

        if step < levels - 1:

            def add(i, carry):
                parts[a][base + i, :, c0:c1] = total(i)
                return carry

            lax.fori_loop(0, size_at[step], add, 0)
            flying[chain] = halve(chain, step + 1)
        else:
            mine = sum(bit_of(order[s]) * size_at[s] for s in range(levels))
            outs[a][mine, :, c0:c1] = total(0)
            flying[chain] = double(chain, 0)

    turns = [
        (step + p[4], chain, step) for chain, p in enumerate(plan) for step in range(2 * levels)
    ]
    for _, chain, step in sorted(turns):
        advance(chain, step)
    for c in sent:
        c.wait_send()


def dp_sum(count, arrays, plan):
    vmem = pl.BlockSpec(memory_space=pltpu.VMEM)
    levels = count.bit_length() - 1
    return pl.pallas_call(
        functools.partial(dp_sum_kernel, count, plan),
        in_specs=[vmem] * len(arrays),
        out_specs=[vmem] * len(arrays),
        out_shape=[jax.ShapeDtypeStruct(a.shape, a.dtype) for a in arrays],
        scratch_shapes=[pltpu.VMEM(a.shape, a.dtype) for a in arrays]
        + [pltpu.SemaphoreType.DMA((len(plan), 2 * levels))] * 2,
        compiler_params=pltpu.CompilerParams(
            collective_id=0, has_side_effects=True, vmem_limit_bytes=VMEM_BYTES
        ),
        name="dp_sum",
    )(*arrays)


def local(
    count,
    inputs, segment_ids, cotangent, attn_norm_gain, attn_norm_bias, qkv_weight, qkv_bias,
    attn_sub_gain, attn_sub_bias, out_weight, out_bias, ffn_norm_gain, ffn_norm_bias,
    up_weight, up_bias, ffn_sub_gain, ffn_sub_bias, down_weight, down_bias,
):
    _, length, width = inputs.shape
    half = qkv_weight.shape[2]
    fhalf = up_weight.shape[1]
    ff = 2 * fhalf
    pairs = width // PAIR
    tiles = length // TILE
    swap = [(0, 1), (1, 0)]

    def trade(a):
        return lax.ppermute(a, "tensor", swap)

    x = inputs[0]
    cot = cotangent[0]
    qkv_other = trade(qkv_weight)
    split = jnp.concatenate(
        [qkv_bias.reshape(-1), attn_sub_gain, attn_sub_bias, up_bias, ffn_sub_gain, ffn_sub_bias]
    )
    split_other = trade(split)
    out_other = trade(out_weight)
    up_other = trade(up_weight)
    down_other = trade(down_weight)

    def joined(start, size):
        return jnp.concatenate([split[start : start + size], split_other[start : start + size]])[None]

    qb = jnp.concatenate(
        [split[: 3 * half].reshape(3, half), split_other[: 3 * half].reshape(3, half)], axis=1
    )
    sg = joined(3 * half, half)
    sb = joined(4 * half, half)
    ub = joined(5 * half, fhalf)
    fg = joined(5 * half + fhalf, fhalf)
    fb = joined(5 * half + 2 * fhalf, fhalf)

    segment = lax.dynamic_slice_in_dim(segment_ids, lax.axis_index("tensor"), 1, 0)[0]
    index = jnp.arange(length, dtype=jnp.int32)
    begins = jnp.concatenate([jnp.ones((1,), jnp.bool_), segment[1:] != segment[:-1]])
    place = index - lax.cummax(jnp.where(begins, index, 0))
    frequency = jnp.exp(
        jnp.arange(HD // 2).astype(F32) * (-2.0 * math.log(10000.0) / HD)
    )
    angle = place.astype(F32)[:, None] * frequency
    cosine, sine = jnp.cos(angle), jnp.sin(angle)
    cos = jnp.concatenate([cosine] * 4, axis=1)
    sin = jnp.concatenate([-sine, sine, -sine, sine], axis=1)
    scol = segment[:, None]
    srow = segment[None, :]

    row = lambda v: v[None]
    mm = 2 * length * width
    normed1, q, k, v = call(
        project_kernel,
        tiles,
        [tiled(x, TILE), fixed(row(attn_norm_gain)), fixed(row(attn_norm_bias)), fixed(qkv_weight),
         fixed(qkv_other), fixed(qb), tiled(cos, TILE), tiled(sin, TILE)],
        [((length, width), BF16, (TILE, width), lambda i: (i, 0))] * 4,
        [],
        3 * mm * width,
        "project",
    )
    spans = sum(b - a for a, b in map(key_range, range(tiles)))
    pair_out = lambda dtype: ((length, width), dtype, (length, PAIR), lambda i: (0, i))
    mixed, lse = call(
        attend_kernel,
        pairs,
        [columns(q), columns(k), columns(v), fixed(scol), fixed(srow)],
        [pair_out(F32), ((pairs, 8, length), F32, (1, 8, length), lambda i: (i, 0, 0))],
        [pltpu.VMEM((TILE, spans), F32)],
        8 * mm * spans // tiles,
        "attend",
    )
    tile_out = lambda w, dtype: ((length, w), dtype, (TILE, w), lambda i: (i, 0))
    vec_out = lambda w: ((1, w), F32, (1, w), lambda i: (0, 0))
    (
        outputs, dmid, dmidb, dmix, sub1, normed2, sub2, dhid,
        g_sg, g_sb, g_ob, g_ng, g_nb, g_ub, g_fg, g_fb, g_db,
    ) = call(
        middle_kernel,
        tiles,
        [tiled(x, TILE), tiled(mixed, TILE), tiled(cot, TILE), fixed(sg), fixed(sb), fixed(out_weight),
         fixed(out_other), fixed(row(out_bias)), fixed(row(ffn_norm_gain)), fixed(row(ffn_norm_bias)),
         fixed(up_weight), fixed(up_other), fixed(ub), fixed(fg), fixed(fb), fixed(down_weight),
         fixed(down_other), fixed(row(down_bias))],
        [tile_out(width, BF16), tile_out(width, F32), tile_out(width, BF16), tile_out(width, BF16),
         tile_out(width, BF16), tile_out(width, BF16), tile_out(ff, BF16), tile_out(ff, BF16),
         vec_out(width), vec_out(width), vec_out(width), vec_out(width), vec_out(width),
         vec_out(ff), vec_out(ff), vec_out(ff), vec_out(width)],
        [pltpu.VMEM((TILE, ff), F32), pltpu.VMEM((TILE, ff), F32)],
        2 * mm * (width + 2 * ff),
        "middle",
    )

    def merged(left, right, left_side):
        size = (left if left_side else right).shape[1] // 2

        def product(start):
            a = left[:, start : start + size] if left_side else left
            b = right if left_side else right[:, start : start + size]
            return tn(a, b)

        return (product(0) + trade(product(size).astype(BF16)).astype(F32)).astype(BF16)

    down_grad = merged(sub2, cot, True)
    up_grad = merged(normed2, dhid, False)
    out_grad = merged(sub1, dmidb, True)
    dq, dk, dv, g_bq, g_bk, g_bv = call(
        attend_back_kernel,
        pairs,
        [columns(q), columns(k), columns(v), columns(dmix),
         (lse, (1, 8, length), lambda i: (i, 0, 0)), fixed(scol), fixed(srow), fixed(cos), fixed(sin)],
        [pair_out(BF16)] * 3 + [((1, width), F32, (1, PAIR), lambda i: (0, i))] * 3,
        [pltpu.VMEM((spans, TILE), F32), pltpu.VMEM((length, PAIR), F32),
         pltpu.VMEM((length, PAIR), F32)],
        20 * mm * spans // tiles,
        "attend_back",
    )
    qkv_grad = [merged(normed1, d, False) for d in (dq, dk, dv)]
    input_grad, g_ag, g_ab = call(
        finish_kernel,
        tiles,
        [tiled(x, TILE), tiled(dmid, TILE), tiled(dq, TILE), tiled(dk, TILE), tiled(dv, TILE),
         fixed(row(attn_norm_gain)), fixed(qkv_weight), fixed(qkv_other)],
        [tile_out(width, F32), vec_out(width), vec_out(width)],
        [],
        3 * mm * width,
        "finish",
    )
    cut = [g_bq, g_bk, g_bv, g_sg, g_sb, g_ub, g_fg, g_fb]
    shared = [g_ag, g_ab, g_ob, g_ng, g_nb, g_db]
    mine = jnp.concatenate([c[0, : c.shape[1] // 2] for c in cut] + [s[0] for s in shared])
    theirs = jnp.concatenate([c[0, c.shape[1] // 2 :] for c in cut] + [s[0] for s in shared])
    small = mine + trade(theirs)
    pad = jnp.zeros((-small.size % (16 * PAIR * count),), F32)
    small = jnp.concatenate([small, pad]).astype(BF16).reshape(count, -1, PAIR)
    out_grad = jnp.concatenate([out_grad[:, :half], out_grad[:, half:]])
    blocks = lambda a: a.reshape(count, a.shape[0] // count, a.shape[1])
    plan = (
        (0, 0, 0, width // 2, 0), (1, 1, 0, fhalf // 2, 0), (2, 2, 0, half, 0), (3, 2, 0, half, 0),
        (0, 0, width // 2, width, 1), (1, 1, fhalf // 2, fhalf, 1), (4, 2, 0, half, 1),
        (5, 2, 0, half, 1), (6, 2, 0, PAIR, 1),
    )
    down_grad, up_grad, *qkv_grad, out_grad, small = dp_sum(
        count, [blocks(a) for a in (down_grad, up_grad, *qkv_grad, out_grad)] + [small], plan
    )
    down_grad = down_grad.reshape(fhalf, width)
    up_grad = up_grad.reshape(width, fhalf)
    qkv_grad = jnp.stack([g.reshape(width, half) for g in qkv_grad]).astype(F32)
    out_grad = out_grad.reshape(width, half)
    out_grad = jnp.concatenate([out_grad[:half], out_grad[half:]], axis=1).astype(F32)
    small = small.reshape(-1).astype(F32)
    pieces = []
    at = 0
    for size in [c.shape[1] // 2 for c in cut] + [s.shape[1] for s in shared]:
        pieces.append(small[at : at + size])
        at += size
    g_bq, g_bk, g_bv, g_sg, g_sb, g_ub, g_fg, g_fb, g_ag, g_ab, g_ob, g_ng, g_nb, g_db = pieces
    return (
        outputs[None], input_grad[None], g_ag, g_ab, qkv_grad, jnp.stack([g_bq, g_bk, g_bv]),
        g_sg, g_sb, out_grad, g_ob, g_ng, g_nb, up_grad.astype(F32), g_ub, g_fg, g_fb,
        down_grad.astype(F32), g_db,
    )


def solution(mesh):
    rows = P(("dp", "tensor"), None, None)
    in_specs = (
        rows, P("dp", None), rows, P(), P(), P(None, None, "tensor"), P(None, "tensor"),
        P("tensor"), P("tensor"), P("tensor", None), P(), P(), P(), P(None, "tensor"),
        P("tensor"), P("tensor"), P("tensor"), P("tensor", None), P(),
    )
    out_specs = (
        rows, rows, P(), P(), P(None, None, "tensor"), P(None, "tensor"), P("tensor"), P("tensor"),
        P("tensor", None), P(), P(), P(), P(None, "tensor"), P("tensor"), P("tensor"), P("tensor"),
        P("tensor", None), P(),
    )
    body = functools.partial(local, mesh.shape["dp"])
    return jax.shard_map(body, mesh=mesh, in_specs=in_specs, out_specs=out_specs, check_vma=False)
```

```python
import functools
import math

import jax
import jax.numpy as jnp
from jax import lax
from jax.experimental import pallas as pl
from jax.experimental.pallas import tpu as pltpu
from jax.sharding import PartitionSpec as P

HD = 64
PAIR = 2 * HD
TILE = 256
REACH = 512
F32 = jnp.float32
BF16 = jnp.bfloat16
VMEM_BYTES = 60 * 1024 * 1024


def nn(a, b):
    return jnp.dot(a, b, preferred_element_type=F32)


def nt(a, b):
    return lax.dot_general(a, b, (((1,), (1,)), ((), ())), preferred_element_type=F32)


def tn(a, b):
    return lax.dot_general(a, b, (((0,), (0,)), ((), ())), preferred_element_type=F32)


def unit_rows(values):
    center = jnp.mean(values, axis=-1, keepdims=True)
    spread = jnp.mean(values * values, axis=-1, keepdims=True) - center * center
    inv = lax.rsqrt(spread + 1e-05)
    return (values - center) * inv, inv


def norm_back(grad, unit, inv, gain):
    scaled = grad * gain
    return inv * (
        scaled
        - jnp.mean(scaled, axis=-1, keepdims=True)
        - unit * jnp.mean(scaled * unit, axis=-1, keepdims=True)
    )


def swap_halves(values):
    lane = lax.broadcasted_iota(jnp.int32, values.shape, 1)
    return jnp.where(
        (lane & (HD // 2)) == 0,
        pltpu.roll(values, PAIR - HD // 2, axis=1),
        pltpu.roll(values, HD // 2, axis=1),
    )


def add_rows(ref, values):
    total = jnp.sum(values, axis=0, keepdims=True)

    @pl.when(pl.program_id(0) == 0)
    def _():
        ref[...] = total

    @pl.when(pl.program_id(0) != 0)
    def _():
        ref[...] += total


def project_kernel(
    x_ref, gain_ref, bias_ref, own_ref, oth_ref, qb_ref, cos_ref, sin_ref, n_ref, q_ref, k_ref, v_ref
):
    unit, _ = unit_rows(x_ref[...].astype(F32))
    normed = (unit * gain_ref[...] + bias_ref[...]).astype(BF16)
    n_ref[...] = normed
    half = own_ref.shape[2]
    cos = cos_ref[...]
    sin = sin_ref[...]
    for j, out_ref in enumerate((q_ref, k_ref, v_ref)):
        for side, w_ref in enumerate((own_ref, oth_ref)):
            pre = nn(normed, w_ref[j]) + qb_ref[j : j + 1, side * half : (side + 1) * half]
            for c in range(half // PAIR):
                part = pre[:, c * PAIR : (c + 1) * PAIR]
                if j < 2:
                    part = part * cos + swap_halves(part) * sin
                part = part.astype(BF16)
                if j == 0:
                    part = part * jnp.asarray(HD**-0.5, BF16)
                at = side * half + c * PAIR
                out_ref[:, at : at + PAIR] = part


def key_range(i):
    return max(0, i * TILE - REACH), (i + 1) * TILE


def head_masks(rows):
    lane = lax.broadcasted_iota(jnp.int32, (rows, PAIR), 1)
    return lane < HD, lane >= HD


def only(mask, values):
    return jnp.where(mask, values, jnp.zeros_like(values))


def fill_bias(scol_ref, srow_ref, bias_ref, blocks):
    at = 0
    for i in range(blocks):
        k0, k1 = key_range(i)
        shape = (k1 - k0, TILE)
        ki = lax.broadcasted_iota(jnp.int32, shape, 0) + k0
        qi = lax.broadcasted_iota(jnp.int32, shape, 1) + i * TILE
        keep = (scol_ref[k0:k1, :] == srow_ref[:, i * TILE : (i + 1) * TILE]) & (qi >= ki)
        bias_ref[at : at + k1 - k0, :] = jnp.where(keep, 0.0, -1e30).astype(F32)
        at += k1 - k0


def attend_kernel(q_ref, k_ref, v_ref, scol_ref, srow_ref, mix_ref, lse_ref, bias_ref):
    blocks = q_ref.shape[0] // TILE

    @pl.when(pl.program_id(0) == 0)
    def _():
        fill_bias(scol_ref, srow_ref, bias_ref, blocks)

    at = 0
    for i in range(blocks):
        k0, k1 = key_range(i)
        width = k1 - k0
        bias = bias_ref[at : at + width, :]
        at += width
        rows = slice(i * TILE, (i + 1) * TILE)
        q = q_ref[rows, :]
        keys = k_ref[k0:k1, :]
        values = v_ref[k0:k1, :]
        qm = head_masks(TILE)
        km = head_masks(width)
        ps, vs = [], []
        for h in range(2):
            scores = nt(keys, only(qm[h], q)) + bias
            peak = jnp.max(scores, axis=0, keepdims=True)
            e = jnp.exp(scores - peak)
            total = jnp.sum(e, axis=0, keepdims=True)
            ps.append((e * (1.0 / total)).astype(BF16))
            vs.append(only(km[h], values))
            lse_ref[0, h : h + 1, rows] = peak + jnp.log(total)
        mix_ref[rows, :] = tn(jnp.concatenate(ps, axis=0), jnp.concatenate(vs, axis=0))


def attend_back_kernel(
    q_ref, k_ref, v_ref, g_ref, lse_ref, scol_ref, srow_ref, cos_ref, sin_ref,
    dq_ref, dk_ref, dv_ref, bq_ref, bk_ref, bv_ref, bias_ref, ka_ref, va_ref,
):
    blocks = q_ref.shape[0] // TILE

    @pl.when(pl.program_id(0) == 0)
    def _():
        fill_bias(scol_ref, srow_ref, bias_ref, blocks)

    ka_ref[...] = jnp.zeros_like(ka_ref)
    va_ref[...] = jnp.zeros_like(va_ref)

    def turn_back(values, rows):
        return values * cos_ref[rows, :] - swap_halves(values) * sin_ref[rows, :]

    sums_q = jnp.zeros((1, PAIR), F32)
    at = 0
    for i in range(blocks):
        k0, k1 = key_range(i)
        width = k1 - k0
        bias = bias_ref[at : at + width, :]
        at += width
        rows = slice(i * TILE, (i + 1) * TILE)
        q = q_ref[rows, :]
        g = g_ref[rows, :]
        keys = k_ref[k0:k1, :]
        values = v_ref[k0:k1, :]
        qm = head_masks(TILE)
        km = head_masks(width)
        qs, gs, ks, ps, ds = [], [], [], [], []
        for h in range(2):
            qh = only(qm[h], q)
            gh = only(qm[h], g)
            scores = nt(keys, qh) + bias
            p = jnp.exp(scores - lse_ref[0, h : h + 1, rows])
            pull = p * nt(values, gh)
            inner = jnp.sum(pull, axis=0, keepdims=True)
            qs.append(qh)
            gs.append(gh)
            ks.append(only(km[h], keys))
            ps.append(p.astype(BF16))
            ds.append((pull - p * inner).astype(BF16))
        q2 = jnp.concatenate(qs, axis=0)
        g2 = jnp.concatenate(gs, axis=0)
        va_ref[k0:k1, :] += nn(jnp.concatenate(ps, axis=1), g2)
        ka_ref[k0:k1, :] += nn(jnp.concatenate(ds, axis=1), q2)
        dq = tn(jnp.concatenate(ds, axis=0), jnp.concatenate(ks, axis=0)) * (HD**-0.5)
        dq = turn_back(dq, rows).astype(BF16)
        dq_ref[rows, :] = dq
        sums_q += jnp.sum(dq.astype(F32), axis=0, keepdims=True)
    bq_ref[...] = sums_q
    dk = turn_back(ka_ref[...], slice(None)).astype(BF16)
    dk_ref[...] = dk
    bk_ref[...] = jnp.sum(dk.astype(F32), axis=0, keepdims=True)
    dv = va_ref[...].astype(BF16)
    dv_ref[...] = dv
    bv_ref[...] = jnp.sum(dv.astype(F32), axis=0, keepdims=True)


def middle_kernel(
    x_ref, mix_ref, cot_ref, sg_ref, sb_ref, wo0_ref, wo1_ref, ob_ref, ng_ref, nb_ref,
    wu0_ref, wu1_ref, ub_ref, fg_ref, fb_ref, wd0_ref, wd1_ref, db_ref,
    out_ref, dmid_ref, dmidb_ref, dmix_ref, sub1_ref, n2_ref, sub2_ref, dhid_ref,
    gsg_ref, gsb_ref, gob_ref, gng_ref, gnb_ref, gub_ref, gfg_ref, gfb_ref, gdb_ref,
    act_ref, slope_ref,
):
    half = wo0_ref.shape[0]
    fhalf = wd0_ref.shape[0]
    ff = 2 * fhalf
    unit1, inv1 = unit_rows(mix_ref[...])
    sub1 = (unit1 * sg_ref[...] + sb_ref[...]).astype(BF16)
    sub1_ref[...] = sub1
    middle = (
        x_ref[...].astype(F32)
        + (nn(sub1[:, :half], wo0_ref[...]) + nn(sub1[:, half:], wo1_ref[...]))
        + ob_ref[...]
    )
    unit2, inv2 = unit_rows(middle)
    normed2 = (unit2 * ng_ref[...] + nb_ref[...]).astype(BF16)
    n2_ref[...] = normed2
    rows = normed2.shape[0]
    total = jnp.zeros((rows, 1), F32)
    square = jnp.zeros((rows, 1), F32)
    step = 512
    for at in range(0, ff, step):
        w_ref, off = (wu0_ref, at) if at < fhalf else (wu1_ref, at - fhalf)
        hidden = nn(normed2, w_ref[:, off : off + step]) + ub_ref[:, at : at + step]
        gate = 0.5 + 0.5 * lax.erf(hidden * (0.5**0.5))
        active = hidden * gate
        act_ref[:, at : at + step] = active
        slope_ref[:, at : at + step] = gate + hidden * (
            jnp.exp(hidden * hidden * -0.5) * (1.0 / math.sqrt(2.0 * math.pi))
        )
        total += jnp.sum(active, axis=-1, keepdims=True)
        square += jnp.sum(active * active, axis=-1, keepdims=True)
    center3 = total * (1.0 / ff)
    inv3 = lax.rsqrt(square * (1.0 / ff) - center3 * center3 + 1e-05)
    cot = cot_ref[...]
    final = middle + db_ref[...]
    t_sum = jnp.zeros((rows, 1), F32)
    t_unit = jnp.zeros((rows, 1), F32)

    def unit3(at):
        return (act_ref[:, at : at + step] - center3) * inv3

    def back2(at):
        w_ref, off = (wd0_ref, at) if at < fhalf else (wd1_ref, at - fhalf)
        return nt(cot, w_ref[off : off + step, :])

    scaled = []
    for at in range(0, ff, step):
        w_ref, off = (wd0_ref, at) if at < fhalf else (wd1_ref, at - fhalf)
        unit = unit3(at)
        act_ref[:, at : at + step] = unit
        sub2 = (unit * fg_ref[:, at : at + step] + fb_ref[:, at : at + step]).astype(BF16)
        sub2_ref[:, at : at + step] = sub2
        final += nn(sub2, w_ref[off : off + step, :])
        grad = back2(at)
        add_rows(gfg_ref.at[:, at : at + step], grad * unit)
        add_rows(gfb_ref.at[:, at : at + step], grad)
        t = grad * fg_ref[:, at : at + step]
        scaled.append(t)
        t_sum += jnp.sum(t, axis=-1, keepdims=True)
        t_unit += jnp.sum(t * unit, axis=-1, keepdims=True)
    out_ref[...] = final.astype(BF16)
    t_sum = t_sum * (1.0 / ff)
    t_unit = t_unit * (1.0 / ff)
    dn2 = jnp.zeros(middle.shape, F32)
    for n, at in enumerate(range(0, ff, step)):
        w_ref, off = (wu0_ref, at) if at < fhalf else (wu1_ref, at - fhalf)
        dact = inv3 * (scaled[n] - t_sum - act_ref[:, at : at + step] * t_unit)
        dhid = (dact * slope_ref[:, at : at + step]).astype(BF16)
        dhid_ref[:, at : at + step] = dhid
        add_rows(gub_ref.at[:, at : at + step], dhid.astype(F32))
        dn2 += nt(dhid, w_ref[:, off : off + step])
    cotf = cot.astype(F32)
    add_rows(gdb_ref, cotf)
    add_rows(gng_ref, dn2 * unit2)
    add_rows(gnb_ref, dn2)
    dmid = cotf + norm_back(dn2, unit2, inv2, ng_ref[...])
    dmid_ref[...] = dmid
    dmidb = dmid.astype(BF16)
    dmidb_ref[...] = dmidb
    add_rows(gob_ref, dmidb.astype(F32))
    ds1 = jnp.concatenate([nt(dmidb, wo0_ref[...]), nt(dmidb, wo1_ref[...])], axis=1)
    add_rows(gsg_ref, ds1 * unit1)
    add_rows(gsb_ref, ds1)
    dmix_ref[...] = norm_back(ds1, unit1, inv1, sg_ref[...]).astype(BF16)


def finish_kernel(
    x_ref, dmid_ref, dq_ref, dk_ref, dv_ref, gain_ref, own_ref, oth_ref, out_ref, gg_ref, gb_ref
):
    half = own_ref.shape[2]
    dn1 = None
    for j, d_ref in enumerate((dq_ref, dk_ref, dv_ref)):
        d = d_ref[...]
        part = nt(d[:, :half], own_ref[j]) + nt(d[:, half:], oth_ref[j])
        dn1 = part if dn1 is None else dn1 + part
    unit, inv = unit_rows(x_ref[...].astype(F32))
    add_rows(gg_ref, dn1 * unit)
    add_rows(gb_ref, dn1)
    out_ref[...] = dmid_ref[...] + norm_back(dn1, unit, inv, gain_ref[...])


def call(kernel, grid, ins, outs, scratch, flops, name):
    moved = sum(a.size * a.dtype.itemsize for a, _, _ in ins)
    moved += sum(math.prod(s) * jnp.dtype(d).itemsize for s, d, _, _ in outs)
    return pl.pallas_call(
        kernel,
        grid=(grid,),
        in_specs=[pl.BlockSpec(b, m) for _, b, m in ins],
        out_specs=[pl.BlockSpec(b, m) for _, _, b, m in outs],
        out_shape=[jax.ShapeDtypeStruct(s, d) for s, d, _, _ in outs],
        scratch_shapes=scratch,
        compiler_params=pltpu.CompilerParams(
            dimension_semantics=("arbitrary",), vmem_limit_bytes=VMEM_BYTES
        ),
        cost_estimate=pl.CostEstimate(flops=flops, bytes_accessed=moved, transcendentals=0),
        name=name,
    )(*[a for a, _, _ in ins])


def fixed(a):
    return (a, a.shape, lambda i, n=a.ndim: (0,) * n)


def tiled(a, tile):
    return (a, (tile, a.shape[1]), lambda i: (i, 0))


def columns(a):
    return (a, (a.shape[0], PAIR), lambda i: (0, i))


def bit_order(count, stream):
    bits = list(range(count.bit_length() - 1))
    turn = min(3, len(bits))
    return bits[stream % turn : turn] + bits[: stream % turn] + bits[turn:]


def dp_sum_kernel(count, plan, *refs):
    arrays = max(p[0] for p in plan) + 1
    ins = refs[:arrays]
    outs = refs[arrays : 2 * arrays]
    parts = refs[2 * arrays : 3 * arrays]
    send_sem, recv_sem = refs[3 * arrays :]
    levels = count.bit_length() - 1
    me = lax.axis_index("dp")
    bit_of = lambda bit: (me // (1 << bit)) % 2
    peer = lambda bit: me + (1 - 2 * bit_of(bit)) * (1 << bit)
    barrier = pltpu.get_barrier_semaphore()
    for bit in range(levels):
        pl.semaphore_signal(
            barrier, inc=1, device_id={"dp": peer(bit)}, device_id_type=pl.DeviceIdType.MESH
        )
    pl.semaphore_wait(barrier, levels)

    def copy(src, dst, chain, step, bit):
        return pltpu.make_async_remote_copy(
            src_ref=src, dst_ref=dst, send_sem=send_sem.at[chain, step],
            recv_sem=recv_sem.at[chain, step], device_id={"dp": peer(bit)},
            device_id_type=pl.DeviceIdType.MESH,
        )

    size_at = [count >> (s + 1) for s in range(levels)]
    base_at = [count - (count >> s) for s in range(levels)]
    sent = []

    def halve(chain, step):
        a, stream, c0, c1 = plan[chain][:4]
        bit = bit_order(count, stream)[step]
        size = size_at[step]
        away = (1 - bit_of(bit)) * size
        if step == 0:
            src = ins[a].at[pl.ds(away, size), :, c0:c1]
        else:
            src = parts[a].at[pl.ds(base_at[step - 1] + away, size), :, c0:c1]
        dst = parts[a].at[pl.ds(base_at[step], size), :, c0:c1]
        c = copy(src, dst, chain, step, bit)
        c.start()
        sent.append(c)
        return c

    starts = {}

    def double(chain, step):
        a, stream, c0, c1 = plan[chain][:4]
        order = bit_order(count, stream)
        level = levels - 1 - step
        first = sum(bit_of(order[s]) * size_at[s] for s in range(level + 1))
        view = outs[a].at[pl.ds(first, size_at[level]), :, c0:c1]
        c = copy(view, view, chain, levels + step, order[level])
        c.start()
        sent.append(c)
        return c

    flying = [halve(chain, 0) for chain in range(len(plan))]

    def advance(chain, step):
        a, stream, c0, c1 = plan[chain][:4]
        flying[chain].wait_recv()
        if step >= levels:
            if step < 2 * levels - 1:
                flying[chain] = double(chain, step - levels + 1)
            return
        order = bit_order(count, stream)
        kept = bit_of(order[step]) * size_at[step]
        base = base_at[step]

        def total(i):
            own = (
                ins[a][kept + i, :, c0:c1]
                if step == 0
                else parts[a][base_at[step - 1] + kept + i, :, c0:c1]
            )
            return (own.astype(F32) + parts[a][base + i, :, c0:c1].astype(F32)).astype(BF16)

        if step < levels - 1:

            def add(i, carry):
                parts[a][base + i, :, c0:c1] = total(i)
                return carry

            lax.fori_loop(0, size_at[step], add, 0)
            flying[chain] = halve(chain, step + 1)
        else:
            mine = sum(bit_of(order[s]) * size_at[s] for s in range(levels))
            outs[a][mine, :, c0:c1] = total(0)
            flying[chain] = double(chain, 0)

    turns = [
        (step + p[4], chain, step) for chain, p in enumerate(plan) for step in range(2 * levels)
    ]
    for _, chain, step in sorted(turns):
        advance(chain, step)
    for c in sent:
        c.wait_send()


def dp_sum(count, arrays, plan):
    vmem = pl.BlockSpec(memory_space=pltpu.VMEM)
    levels = count.bit_length() - 1
    return pl.pallas_call(
        functools.partial(dp_sum_kernel, count, plan),
        in_specs=[vmem] * len(arrays),
        out_specs=[vmem] * len(arrays),
        out_shape=[jax.ShapeDtypeStruct(a.shape, a.dtype) for a in arrays],
        scratch_shapes=[pltpu.VMEM(a.shape, a.dtype) for a in arrays]
        + [pltpu.SemaphoreType.DMA((len(plan), 2 * levels))] * 2,
        compiler_params=pltpu.CompilerParams(
            collective_id=0, has_side_effects=True, vmem_limit_bytes=VMEM_BYTES
        ),
        name="dp_sum",
    )(*arrays)


def local(
    count,
    inputs, segment_ids, cotangent, attn_norm_gain, attn_norm_bias, qkv_weight, qkv_bias,
    attn_sub_gain, attn_sub_bias, out_weight, out_bias, ffn_norm_gain, ffn_norm_bias,
    up_weight, up_bias, ffn_sub_gain, ffn_sub_bias, down_weight, down_bias,
):
    _, length, width = inputs.shape
    half = qkv_weight.shape[2]
    fhalf = up_weight.shape[1]
    ff = 2 * fhalf
    pairs = width // PAIR
    tiles = length // TILE
    swap = [(0, 1), (1, 0)]

    def trade(a):
        return lax.ppermute(a, "tensor", swap)

    x = inputs[0]
    cot = cotangent[0]
    qkv_other = trade(qkv_weight)
    split = jnp.concatenate(
        [qkv_bias.reshape(-1), attn_sub_gain, attn_sub_bias, up_bias, ffn_sub_gain, ffn_sub_bias]
    )
    split_other = trade(split)
    out_other = trade(out_weight)
    up_other = trade(up_weight)
    down_other = trade(down_weight)

    def joined(start, size):
        return jnp.concatenate([split[start : start + size], split_other[start : start + size]])[None]

    qb = jnp.concatenate(
        [split[: 3 * half].reshape(3, half), split_other[: 3 * half].reshape(3, half)], axis=1
    )
    sg = joined(3 * half, half)
    sb = joined(4 * half, half)
    ub = joined(5 * half, fhalf)
    fg = joined(5 * half + fhalf, fhalf)
    fb = joined(5 * half + 2 * fhalf, fhalf)

    segment = lax.dynamic_slice_in_dim(segment_ids, lax.axis_index("tensor"), 1, 0)[0]
    index = jnp.arange(length, dtype=jnp.int32)
    begins = jnp.concatenate([jnp.ones((1,), jnp.bool_), segment[1:] != segment[:-1]])
    place = index - lax.cummax(jnp.where(begins, index, 0))
    frequency = jnp.exp(
        jnp.arange(HD // 2).astype(F32) * (-2.0 * math.log(10000.0) / HD)
    )
    angle = place.astype(F32)[:, None] * frequency
    cosine, sine = jnp.cos(angle), jnp.sin(angle)
    cos = jnp.concatenate([cosine] * 4, axis=1)
    sin = jnp.concatenate([-sine, sine, -sine, sine], axis=1)
    scol = segment[:, None]
    srow = segment[None, :]

    row = lambda v: v[None]
    mm = 2 * length * width
    normed1, q, k, v = call(
        project_kernel,
        tiles,
        [tiled(x, TILE), fixed(row(attn_norm_gain)), fixed(row(attn_norm_bias)), fixed(qkv_weight),
         fixed(qkv_other), fixed(qb), tiled(cos, TILE), tiled(sin, TILE)],
        [((length, width), BF16, (TILE, width), lambda i: (i, 0))] * 4,
        [],
        3 * mm * width,
        "project",
    )
    spans = sum(b - a for a, b in map(key_range, range(tiles)))
    pair_out = lambda dtype: ((length, width), dtype, (length, PAIR), lambda i: (0, i))
    mixed, lse = call(
        attend_kernel,
        pairs,
        [columns(q), columns(k), columns(v), fixed(scol), fixed(srow)],
        [pair_out(F32), ((pairs, 8, length), F32, (1, 8, length), lambda i: (i, 0, 0))],
        [pltpu.VMEM((spans, TILE), F32)],
        8 * mm * spans // tiles,
        "attend",
    )
    tile_out = lambda w, dtype: ((length, w), dtype, (TILE, w), lambda i: (i, 0))
    vec_out = lambda w: ((1, w), F32, (1, w), lambda i: (0, 0))
    (
        outputs, dmid, dmidb, dmix, sub1, normed2, sub2, dhid,
        g_sg, g_sb, g_ob, g_ng, g_nb, g_ub, g_fg, g_fb, g_db,
    ) = call(
        middle_kernel,
        tiles,
        [tiled(x, TILE), tiled(mixed, TILE), tiled(cot, TILE), fixed(sg), fixed(sb), fixed(out_weight),
         fixed(out_other), fixed(row(out_bias)), fixed(row(ffn_norm_gain)), fixed(row(ffn_norm_bias)),
         fixed(up_weight), fixed(up_other), fixed(ub), fixed(fg), fixed(fb), fixed(down_weight),
         fixed(down_other), fixed(row(down_bias))],
        [tile_out(width, BF16), tile_out(width, F32), tile_out(width, BF16), tile_out(width, BF16),
         tile_out(width, BF16), tile_out(width, BF16), tile_out(ff, BF16), tile_out(ff, BF16),
         vec_out(width), vec_out(width), vec_out(width), vec_out(width), vec_out(width),
         vec_out(ff), vec_out(ff), vec_out(ff), vec_out(width)],
        [pltpu.VMEM((TILE, ff), F32), pltpu.VMEM((TILE, ff), F32)],
        2 * mm * (width + 2 * ff),
        "middle",
    )

    def merged(left, right, left_side):
        size = (left if left_side else right).shape[1] // 2

        def product(start):
            a = left[:, start : start + size] if left_side else left
            b = right if left_side else right[:, start : start + size]
            return tn(a, b)

        return (product(0) + trade(product(size).astype(BF16)).astype(F32)).astype(BF16)

    down_grad = merged(sub2, cot, True)
    dmix, down_grad = lax.optimization_barrier((dmix, down_grad))
    down_grad = lax.psum(down_grad, "dp")
    up_grad = merged(normed2, dhid, False)
    out_grad = merged(sub1, dmidb, True)
    dq, dk, dv, g_bq, g_bk, g_bv = call(
        attend_back_kernel,
        pairs,
        [columns(q), columns(k), columns(v), columns(dmix),
         (lse, (1, 8, length), lambda i: (i, 0, 0)), fixed(scol), fixed(srow), fixed(cos), fixed(sin)],
        [pair_out(BF16)] * 3 + [((1, width), F32, (1, PAIR), lambda i: (0, i))] * 3,
        [pltpu.VMEM((spans, TILE), F32), pltpu.VMEM((length, PAIR), F32),
         pltpu.VMEM((length, PAIR), F32)],
        20 * mm * spans // tiles,
        "attend_back",
    )
    qkv_grad = [merged(normed1, d, False) for d in (dq, dk, dv)]
    input_grad, g_ag, g_ab = call(
        finish_kernel,
        tiles,
        [tiled(x, TILE), tiled(dmid, TILE), tiled(dq, TILE), tiled(dk, TILE), tiled(dv, TILE),
         fixed(row(attn_norm_gain)), fixed(qkv_weight), fixed(qkv_other)],
        [tile_out(width, F32), vec_out(width), vec_out(width)],
        [],
        3 * mm * width,
        "finish",
    )
    cut = [g_bq, g_bk, g_bv, g_sg, g_sb, g_ub, g_fg, g_fb]
    shared = [g_ag, g_ab, g_ob, g_ng, g_nb, g_db]
    mine = jnp.concatenate([c[0, : c.shape[1] // 2] for c in cut] + [s[0] for s in shared])
    theirs = jnp.concatenate([c[0, c.shape[1] // 2 :] for c in cut] + [s[0] for s in shared])
    small = mine + trade(theirs)
    pad = jnp.zeros((-small.size % (16 * PAIR * count),), F32)
    small = jnp.concatenate([small, pad]).astype(BF16).reshape(count, -1, PAIR)
    out_grad = jnp.concatenate([out_grad[:, :half], out_grad[:, half:]])
    blocks = lambda a: a.reshape(count, a.shape[0] // count, a.shape[1])
    third = fhalf // 3
    side = half // 3
    plan = (
        (0, 0, 0, third, 0), (0, 1, 2 * third, fhalf, 0), (2, 2, 0, half, 0),
        (4, 2, side, 2 * side, 0),
        (0, 0, third, 2 * third, 1), (1, 1, 0, half, 1), (4, 1, 0, side, 1), (3, 2, 0, half, 1),
        (4, 2, 2 * side, half, 1), (5, 1, 0, PAIR, 1),
    )
    up_grad, *qkv_grad, out_grad, small = dp_sum(
        count, [blocks(a) for a in (up_grad, *qkv_grad, out_grad)] + [small], plan
    )
    up_grad = up_grad.reshape(width, fhalf)
    qkv_grad = jnp.stack([g.reshape(width, half) for g in qkv_grad]).astype(F32)
    out_grad = out_grad.reshape(width, half)
    out_grad = jnp.concatenate([out_grad[:half], out_grad[half:]], axis=1).astype(F32)
    small = small.reshape(-1).astype(F32)
    pieces = []
    at = 0
    for size in [c.shape[1] // 2 for c in cut] + [s.shape[1] for s in shared]:
        pieces.append(small[at : at + size])
        at += size
    g_bq, g_bk, g_bv, g_sg, g_sb, g_ub, g_fg, g_fb, g_ag, g_ab, g_ob, g_ng, g_nb, g_db = pieces
    return (
        outputs[None], input_grad[None], g_ag, g_ab, qkv_grad, jnp.stack([g_bq, g_bk, g_bv]),
        g_sg, g_sb, out_grad, g_ob, g_ng, g_nb, up_grad.astype(F32), g_ub, g_fg, g_fb,
        down_grad.astype(F32), g_db,
    )


def solution(mesh):
    rows = P(("dp", "tensor"), None, None)
    in_specs = (
        rows, P("dp", None), rows, P(), P(), P(None, None, "tensor"), P(None, "tensor"),
        P("tensor"), P("tensor"), P("tensor", None), P(), P(), P(), P(None, "tensor"),
        P("tensor"), P("tensor"), P("tensor"), P("tensor", None), P(),
    )
    out_specs = (
        rows, rows, P(), P(), P(None, None, "tensor"), P(None, "tensor"), P("tensor"), P("tensor"),
        P("tensor", None), P(), P(), P(), P(None, "tensor"), P("tensor"), P("tensor"), P("tensor"),
        P("tensor", None), P(),
    )
    body = functools.partial(local, mesh.shape["dp"])
    return jax.shard_map(body, mesh=mesh, in_specs=in_specs, out_specs=out_specs, check_vma=False)
```

```python
import functools
import math

import jax
import jax.numpy as jnp
from jax import lax
from jax.experimental import pallas as pl
from jax.experimental.pallas import tpu as pltpu
from jax.sharding import PartitionSpec as P

HD = 64
PAIR = 2 * HD
TILE = 256
REACH = 512
F32 = jnp.float32
BF16 = jnp.bfloat16
VMEM_BYTES = 60 * 1024 * 1024


def flat(ref):
    return ref[...].reshape(1, ref.shape[-1])


def nn(a, b):
    return jnp.dot(a, b, preferred_element_type=F32)


def nt(a, b):
    return lax.dot_general(a, b, (((1,), (1,)), ((), ())), preferred_element_type=F32)


def tn(a, b):
    return lax.dot_general(a, b, (((0,), (0,)), ((), ())), preferred_element_type=F32)


def unit_rows(values):
    center = jnp.mean(values, axis=-1, keepdims=True)
    spread = jnp.mean(values * values, axis=-1, keepdims=True) - center * center
    inv = lax.rsqrt(spread + 1e-05)
    return (values - center) * inv, inv


def norm_back(grad, unit, inv, gain):
    scaled = grad * gain
    return inv * (
        scaled
        - jnp.mean(scaled, axis=-1, keepdims=True)
        - unit * jnp.mean(scaled * unit, axis=-1, keepdims=True)
    )


def swap_halves(values):
    lane = lax.broadcasted_iota(jnp.int32, values.shape, 1)
    return jnp.where(
        (lane & (HD // 2)) == 0,
        pltpu.roll(values, PAIR - HD // 2, axis=1),
        pltpu.roll(values, HD // 2, axis=1),
    )


def add_rows(ref, values):
    total = jnp.sum(values, axis=0, keepdims=True)

    @pl.when(pl.program_id(0) == 0)
    def _():
        ref[...] = total

    @pl.when(pl.program_id(0) != 0)
    def _():
        ref[...] += total


def project_kernel(
    x_ref, gain_ref, bias_ref, own_ref, oth_ref, qb_ref, cos_ref, sin_ref, n_ref, q_ref, k_ref, v_ref
):
    unit, _ = unit_rows(x_ref[...].astype(F32))
    normed = (unit * flat(gain_ref) + flat(bias_ref)).astype(BF16)
    n_ref[...] = normed
    half = own_ref.shape[2]
    cos = cos_ref[...]
    sin = sin_ref[...]
    for j, out_ref in enumerate((q_ref, k_ref, v_ref)):
        for side, w_ref in enumerate((own_ref, oth_ref)):
            pre = nn(normed, w_ref[j]) + qb_ref[j : j + 1, side * half : (side + 1) * half]
            for c in range(half // PAIR):
                part = pre[:, c * PAIR : (c + 1) * PAIR]
                if j < 2:
                    part = part * cos + swap_halves(part) * sin
                part = part.astype(BF16)
                if j == 0:
                    part = part * jnp.asarray(HD**-0.5, BF16)
                at = side * half + c * PAIR
                out_ref[:, at : at + PAIR] = part


def key_range(i):
    return max(0, i * TILE - REACH), (i + 1) * TILE


def head_masks(rows):
    lane = lax.broadcasted_iota(jnp.int32, (rows, PAIR), 1)
    return lane < HD, lane >= HD


def only(mask, values):
    return jnp.where(mask, values, jnp.zeros_like(values))


def fill_bias(scol_ref, srow_ref, bias_ref, blocks):
    at = 0
    for i in range(blocks):
        k0, k1 = key_range(i)
        shape = (k1 - k0, TILE)
        ki = lax.broadcasted_iota(jnp.int32, shape, 0) + k0
        qi = lax.broadcasted_iota(jnp.int32, shape, 1) + i * TILE
        keep = (scol_ref[k0:k1, :] == srow_ref[:, i * TILE : (i + 1) * TILE]) & (qi >= ki)
        bias_ref[at : at + k1 - k0, :] = jnp.where(keep, 0.0, -1e30).astype(F32)
        at += k1 - k0


def attend_kernel(q_ref, k_ref, v_ref, scol_ref, srow_ref, mix_ref, lse_ref, bias_ref):
    blocks = q_ref.shape[0] // TILE

    @pl.when(pl.program_id(0) == 0)
    def _():
        fill_bias(scol_ref, srow_ref, bias_ref, blocks)

    at = 0
    for i in range(blocks):
        k0, k1 = key_range(i)
        width = k1 - k0
        bias = bias_ref[at : at + width, :]
        at += width
        rows = slice(i * TILE, (i + 1) * TILE)
        q = q_ref[rows, :]
        keys = k_ref[k0:k1, :]
        values = v_ref[k0:k1, :]
        qm = head_masks(TILE)
        km = head_masks(width)
        ps, vs = [], []
        for h in range(2):
            scores = nt(keys, only(qm[h], q)) + bias
            peak = jnp.max(scores, axis=0, keepdims=True)
            e = jnp.exp(scores - peak)
            total = jnp.sum(e, axis=0, keepdims=True)
            ps.append((e * (1.0 / total)).astype(BF16))
            vs.append(only(km[h], values))
            lse_ref[0, h : h + 1, rows] = peak + jnp.log(total)
        mix_ref[rows, :] = tn(jnp.concatenate(ps, axis=0), jnp.concatenate(vs, axis=0))


def attend_back_kernel(
    q_ref, k_ref, v_ref, g_ref, lse_ref, scol_ref, srow_ref, cos_ref, sin_ref,
    dq_ref, dk_ref, dv_ref, bq_ref, bk_ref, bv_ref, bias_ref, ka_ref, va_ref,
):
    blocks = q_ref.shape[0] // TILE

    @pl.when(pl.program_id(0) == 0)
    def _():
        fill_bias(scol_ref, srow_ref, bias_ref, blocks)

    ka_ref[...] = jnp.zeros_like(ka_ref)
    va_ref[...] = jnp.zeros_like(va_ref)

    def turn_back(values, rows):
        return values * cos_ref[rows, :] - swap_halves(values) * sin_ref[rows, :]

    sums_q = jnp.zeros((1, PAIR), F32)
    at = 0
    for i in range(blocks):
        k0, k1 = key_range(i)
        width = k1 - k0
        bias = bias_ref[at : at + width, :]
        at += width
        rows = slice(i * TILE, (i + 1) * TILE)
        q = q_ref[rows, :]
        g = g_ref[rows, :]
        keys = k_ref[k0:k1, :]
        values = v_ref[k0:k1, :]
        qm = head_masks(TILE)
        km = head_masks(width)
        qs, gs, ks, ps, ds = [], [], [], [], []
        for h in range(2):
            qh = only(qm[h], q)
            gh = only(qm[h], g)
            scores = nt(keys, qh) + bias
            p = jnp.exp(scores - lse_ref[0, h : h + 1, rows])
            pull = p * nt(values, gh)
            inner = jnp.sum(pull, axis=0, keepdims=True)
            qs.append(qh)
            gs.append(gh)
            ks.append(only(km[h], keys))
            ps.append(p.astype(BF16))
            ds.append((pull - p * inner).astype(BF16))
        q2 = jnp.concatenate(qs, axis=0)
        g2 = jnp.concatenate(gs, axis=0)
        va_ref[k0:k1, :] += nn(jnp.concatenate(ps, axis=1), g2)
        ka_ref[k0:k1, :] += nn(jnp.concatenate(ds, axis=1), q2)
        dq = tn(jnp.concatenate(ds, axis=0), jnp.concatenate(ks, axis=0)) * (HD**-0.5)
        dq = turn_back(dq, rows).astype(BF16)
        dq_ref[rows, :] = dq
        sums_q += jnp.sum(dq.astype(F32), axis=0, keepdims=True)
    bq_ref[...] = sums_q
    dk = turn_back(ka_ref[...], slice(None)).astype(BF16)
    dk_ref[...] = dk
    bk_ref[...] = jnp.sum(dk.astype(F32), axis=0, keepdims=True)
    dv = va_ref[...].astype(BF16)
    dv_ref[...] = dv
    bv_ref[...] = jnp.sum(dv.astype(F32), axis=0, keepdims=True)


def middle_kernel(
    x_ref, mix_ref, cot_ref, sg_ref, sb_ref, wo0_ref, wo1_ref, ob_ref, ng_ref, nb_ref,
    wu0_ref, wu1_ref, ub_ref, fg_ref, fb_ref, wd0_ref, wd1_ref, db_ref,
    out_ref, dmid_ref, dmidb_ref, dmix_ref, sub1_ref, n2_ref, sub2_ref, dhid_ref,
    gsg_ref, gsb_ref, gob_ref, gng_ref, gnb_ref, gub_ref, gfg_ref, gfb_ref, gdb_ref,
    act_ref, slope_ref,
):
    half = wo0_ref.shape[0]
    fhalf = wd0_ref.shape[0]
    ff = 2 * fhalf
    unit1, inv1 = unit_rows(mix_ref[...])
    sub1 = (unit1 * sg_ref[...] + sb_ref[...]).astype(BF16)
    sub1_ref[...] = sub1
    middle = (
        x_ref[...].astype(F32)
        + (nn(sub1[:, :half], wo0_ref[...]) + nn(sub1[:, half:], wo1_ref[...]))
        + flat(ob_ref)
    )
    unit2, inv2 = unit_rows(middle)
    normed2 = (unit2 * flat(ng_ref) + flat(nb_ref)).astype(BF16)
    n2_ref[...] = normed2
    rows = normed2.shape[0]
    total = jnp.zeros((rows, 1), F32)
    square = jnp.zeros((rows, 1), F32)
    step = 512
    for at in range(0, ff, step):
        w_ref, off = (wu0_ref, at) if at < fhalf else (wu1_ref, at - fhalf)
        hidden = nn(normed2, w_ref[:, off : off + step]) + ub_ref[:, at : at + step]
        gate = 0.5 + 0.5 * lax.erf(hidden * (0.5**0.5))
        active = hidden * gate
        act_ref[:, at : at + step] = active
        slope_ref[:, at : at + step] = gate + hidden * (
            jnp.exp(hidden * hidden * -0.5) * (1.0 / math.sqrt(2.0 * math.pi))
        )
        total += jnp.sum(active, axis=-1, keepdims=True)
        square += jnp.sum(active * active, axis=-1, keepdims=True)
    center3 = total * (1.0 / ff)
    inv3 = lax.rsqrt(square * (1.0 / ff) - center3 * center3 + 1e-05)
    cot = cot_ref[...]
    final = middle + flat(db_ref)
    t_sum = jnp.zeros((rows, 1), F32)
    t_unit = jnp.zeros((rows, 1), F32)

    def unit3(at):
        return (act_ref[:, at : at + step] - center3) * inv3

    def back2(at):
        w_ref, off = (wd0_ref, at) if at < fhalf else (wd1_ref, at - fhalf)
        return nt(cot, w_ref[off : off + step, :])

    scaled = []
    for at in range(0, ff, step):
        w_ref, off = (wd0_ref, at) if at < fhalf else (wd1_ref, at - fhalf)
        unit = unit3(at)
        act_ref[:, at : at + step] = unit
        sub2 = (unit * fg_ref[:, at : at + step] + fb_ref[:, at : at + step]).astype(BF16)
        sub2_ref[:, at : at + step] = sub2
        final += nn(sub2, w_ref[off : off + step, :])
        grad = back2(at)
        add_rows(gfg_ref.at[:, at : at + step], grad * unit)
        add_rows(gfb_ref.at[:, at : at + step], grad)
        t = grad * fg_ref[:, at : at + step]
        scaled.append(t)
        t_sum += jnp.sum(t, axis=-1, keepdims=True)
        t_unit += jnp.sum(t * unit, axis=-1, keepdims=True)
    out_ref[...] = final.astype(BF16)
    t_sum = t_sum * (1.0 / ff)
    t_unit = t_unit * (1.0 / ff)
    dn2 = jnp.zeros(middle.shape, F32)
    for n, at in enumerate(range(0, ff, step)):
        w_ref, off = (wu0_ref, at) if at < fhalf else (wu1_ref, at - fhalf)
        dact = inv3 * (scaled[n] - t_sum - act_ref[:, at : at + step] * t_unit)
        dhid = (dact * slope_ref[:, at : at + step]).astype(BF16)
        dhid_ref[:, at : at + step] = dhid
        add_rows(gub_ref.at[:, at : at + step], dhid.astype(F32))
        dn2 += nt(dhid, w_ref[:, off : off + step])
    cotf = cot.astype(F32)
    add_rows(gdb_ref, cotf)
    add_rows(gng_ref, dn2 * unit2)
    add_rows(gnb_ref, dn2)
    dmid = cotf + norm_back(dn2, unit2, inv2, flat(ng_ref))
    dmid_ref[...] = dmid
    dmidb = dmid.astype(BF16)
    dmidb_ref[...] = dmidb
    add_rows(gob_ref, dmidb.astype(F32))
    ds1 = jnp.concatenate([nt(dmidb, wo0_ref[...]), nt(dmidb, wo1_ref[...])], axis=1)
    add_rows(gsg_ref, ds1 * unit1)
    add_rows(gsb_ref, ds1)
    dmix_ref[...] = norm_back(ds1, unit1, inv1, sg_ref[...]).astype(BF16)


def finish_kernel(
    x_ref, dmid_ref, dq_ref, dk_ref, dv_ref, gain_ref, own_ref, oth_ref, out_ref, gg_ref, gb_ref
):
    half = own_ref.shape[2]
    dn1 = None
    for j, d_ref in enumerate((dq_ref, dk_ref, dv_ref)):
        d = d_ref[...]
        part = nt(d[:, :half], own_ref[j]) + nt(d[:, half:], oth_ref[j])
        dn1 = part if dn1 is None else dn1 + part
    unit, inv = unit_rows(x_ref[...].astype(F32))
    add_rows(gg_ref, dn1 * unit)
    add_rows(gb_ref, dn1)
    out_ref[...] = dmid_ref[...] + norm_back(dn1, unit, inv, flat(gain_ref))


def call(kernel, grid, ins, outs, scratch, flops, name):
    moved = sum(a.size * a.dtype.itemsize for a, _, _ in ins)
    moved += sum(math.prod(s) * jnp.dtype(d).itemsize for s, d, _, _ in outs)
    return pl.pallas_call(
        kernel,
        grid=(grid,),
        in_specs=[pl.BlockSpec(b, m) for _, b, m in ins],
        out_specs=[pl.BlockSpec(b, m) for _, _, b, m in outs],
        out_shape=[jax.ShapeDtypeStruct(s, d) for s, d, _, _ in outs],
        scratch_shapes=scratch,
        compiler_params=pltpu.CompilerParams(
            dimension_semantics=("arbitrary",), vmem_limit_bytes=VMEM_BYTES
        ),
        cost_estimate=pl.CostEstimate(flops=flops, bytes_accessed=moved, transcendentals=0),
        name=name,
    )(*[a for a, _, _ in ins])


def fixed(a):
    return (a, a.shape, lambda i, n=a.ndim: (0,) * n)


def tiled(a, tile):
    return (a, (tile, a.shape[1]), lambda i: (i, 0))


def columns(a):
    return (a, (a.shape[0], PAIR), lambda i: (0, i))


def bit_order(count, stream):
    bits = list(range(count.bit_length() - 1))
    turn = min(3, len(bits))
    return bits[stream % turn : turn] + bits[: stream % turn] + bits[turn:]


def dp_sum_kernel(count, plan, *refs):
    arrays = max(p[0] for p in plan) + 1
    ins = refs[:arrays]
    outs = refs[arrays : 2 * arrays]
    parts = refs[2 * arrays : 3 * arrays]
    send_sem, recv_sem = refs[3 * arrays :]
    levels = count.bit_length() - 1
    me = lax.axis_index("dp")
    bit_of = lambda bit: (me // (1 << bit)) % 2
    peer = lambda bit: me + (1 - 2 * bit_of(bit)) * (1 << bit)
    barrier = pltpu.get_barrier_semaphore()
    for bit in range(levels):
        pl.semaphore_signal(
            barrier, inc=1, device_id={"dp": peer(bit)}, device_id_type=pl.DeviceIdType.MESH
        )
    pl.semaphore_wait(barrier, levels)

    def copy(src, dst, chain, step, bit):
        return pltpu.make_async_remote_copy(
            src_ref=src, dst_ref=dst, send_sem=send_sem.at[chain, step],
            recv_sem=recv_sem.at[chain, step], device_id={"dp": peer(bit)},
            device_id_type=pl.DeviceIdType.MESH,
        )

    size_at = [count >> (s + 1) for s in range(levels)]
    base_at = [count - (count >> s) for s in range(levels)]
    sent = []

    def halve(chain, step):
        a, stream, c0, c1 = plan[chain][:4]
        bit = bit_order(count, stream)[step]
        size = size_at[step]
        away = (1 - bit_of(bit)) * size
        if step == 0:
            src = ins[a].at[pl.ds(away, size), :, c0:c1]
        else:
            src = parts[a].at[pl.ds(base_at[step - 1] + away, size), :, c0:c1]
        dst = parts[a].at[pl.ds(base_at[step], size), :, c0:c1]
        c = copy(src, dst, chain, step, bit)
        c.start()
        sent.append(c)
        return c

    starts = {}

    def double(chain, step):
        a, stream, c0, c1 = plan[chain][:4]
        order = bit_order(count, stream)
        level = levels - 1 - step
        first = sum(bit_of(order[s]) * size_at[s] for s in range(level + 1))
        view = outs[a].at[pl.ds(first, size_at[level]), :, c0:c1]
        c = copy(view, view, chain, levels + step, order[level])
        c.start()
        sent.append(c)
        return c

    flying = [halve(chain, 0) for chain in range(len(plan))]

    def advance(chain, step):
        a, stream, c0, c1 = plan[chain][:4]
        flying[chain].wait_recv()
        if step >= levels:
            if step < 2 * levels - 1:
                flying[chain] = double(chain, step - levels + 1)
            return
        order = bit_order(count, stream)
        kept = bit_of(order[step]) * size_at[step]
        base = base_at[step]

        def total(i):
            own = (
                ins[a][kept + i, :, c0:c1]
                if step == 0
                else parts[a][base_at[step - 1] + kept + i, :, c0:c1]
            )
            return (own.astype(F32) + parts[a][base + i, :, c0:c1].astype(F32)).astype(BF16)

        if step < levels - 1:

            def add(i, carry):
                parts[a][base + i, :, c0:c1] = total(i)
                return carry

            lax.fori_loop(0, size_at[step], add, 0)
            flying[chain] = halve(chain, step + 1)
        else:
            mine = sum(bit_of(order[s]) * size_at[s] for s in range(levels))
            outs[a][mine, :, c0:c1] = total(0)
            flying[chain] = double(chain, 0)

    turns = [
        (step + p[4], chain, step) for chain, p in enumerate(plan) for step in range(2 * levels)
    ]
    for _, chain, step in sorted(turns):
        advance(chain, step)
    for c in sent:
        c.wait_send()


def dp_sum(count, arrays, plan):
    vmem = pl.BlockSpec(memory_space=pltpu.VMEM)
    levels = count.bit_length() - 1
    return pl.pallas_call(
        functools.partial(dp_sum_kernel, count, plan),
        in_specs=[vmem] * len(arrays),
        out_specs=[vmem] * len(arrays),
        out_shape=[jax.ShapeDtypeStruct(a.shape, a.dtype) for a in arrays],
        scratch_shapes=[pltpu.VMEM(a.shape, a.dtype) for a in arrays]
        + [pltpu.SemaphoreType.DMA((len(plan), 2 * levels))] * 2,
        compiler_params=pltpu.CompilerParams(
            collective_id=0, has_side_effects=True, vmem_limit_bytes=VMEM_BYTES
        ),
        name="dp_sum",
    )(*arrays)


def local(
    count,
    inputs, segment_ids, cotangent, attn_norm_gain, attn_norm_bias, qkv_weight, qkv_bias,
    attn_sub_gain, attn_sub_bias, out_weight, out_bias, ffn_norm_gain, ffn_norm_bias,
    up_weight, up_bias, ffn_sub_gain, ffn_sub_bias, down_weight, down_bias,
):
    _, length, width = inputs.shape
    half = qkv_weight.shape[2]
    fhalf = up_weight.shape[1]
    ff = 2 * fhalf
    pairs = width // PAIR
    tiles = length // TILE
    swap = [(0, 1), (1, 0)]

    def trade(a):
        return lax.ppermute(a, "tensor", swap)

    x = inputs[0]
    cot = cotangent[0]
    qkv_other = trade(qkv_weight)
    split = jnp.concatenate(
        [qkv_bias.reshape(-1), attn_sub_gain, attn_sub_bias, up_bias, ffn_sub_gain, ffn_sub_bias]
    )
    split_other = trade(split)
    out_other = trade(out_weight)
    up_other = trade(up_weight)
    down_other = trade(down_weight)

    def joined(start, size):
        return jnp.concatenate([split[start : start + size], split_other[start : start + size]])[None]

    qb = jnp.concatenate(
        [split[: 3 * half].reshape(3, half), split_other[: 3 * half].reshape(3, half)], axis=1
    )
    sg = joined(3 * half, half)
    sb = joined(4 * half, half)
    ub = joined(5 * half, fhalf)
    fg = joined(5 * half + fhalf, fhalf)
    fb = joined(5 * half + 2 * fhalf, fhalf)

    segment = lax.dynamic_slice_in_dim(segment_ids, lax.axis_index("tensor"), 1, 0)[0]
    index = jnp.arange(length, dtype=jnp.int32)
    begins = jnp.concatenate([jnp.ones((1,), jnp.bool_), segment[1:] != segment[:-1]])
    place = index - lax.cummax(jnp.where(begins, index, 0))
    frequency = jnp.exp(
        jnp.arange(HD // 2).astype(F32) * (-2.0 * math.log(10000.0) / HD)
    )
    angle = place.astype(F32)[:, None] * frequency
    cosine, sine = jnp.cos(angle), jnp.sin(angle)
    cos = jnp.concatenate([cosine] * 4, axis=1)
    sin = jnp.concatenate([-sine, sine, -sine, sine], axis=1)
    scol = segment[:, None]
    srow = segment[None, :]

    mm = 2 * length * width
    normed1, q, k, v = call(
        project_kernel,
        tiles,
        [tiled(x, TILE), fixed((attn_norm_gain)), fixed((attn_norm_bias)), fixed(qkv_weight),
         fixed(qkv_other), fixed(qb), tiled(cos, TILE), tiled(sin, TILE)],
        [((length, width), BF16, (TILE, width), lambda i: (i, 0))] * 4,
        [],
        3 * mm * width,
        "project",
    )
    spans = sum(b - a for a, b in map(key_range, range(tiles)))
    pair_out = lambda dtype: ((length, width), dtype, (length, PAIR), lambda i: (0, i))
    mixed, lse = call(
        attend_kernel,
        pairs,
        [columns(q), columns(k), columns(v), fixed(scol), fixed(srow)],
        [pair_out(F32), ((pairs, 8, length), F32, (1, 8, length), lambda i: (i, 0, 0))],
        [pltpu.VMEM((spans, TILE), F32)],
        8 * mm * spans // tiles,
        "attend",
    )
    tile_out = lambda w, dtype: ((length, w), dtype, (TILE, w), lambda i: (i, 0))
    vec_out = lambda w: ((1, w), F32, (1, w), lambda i: (0, 0))
    (
        outputs, dmid, dmidb, dmix, sub1, normed2, sub2, dhid,
        g_sg, g_sb, g_ob, g_ng, g_nb, g_ub, g_fg, g_fb, g_db,
    ) = call(
        middle_kernel,
        tiles,
        [tiled(x, TILE), tiled(mixed, TILE), tiled(cot, TILE), fixed(sg), fixed(sb), fixed(out_weight),
         fixed(out_other), fixed((out_bias)), fixed((ffn_norm_gain)), fixed((ffn_norm_bias)),
         fixed(up_weight), fixed(up_other), fixed(ub), fixed(fg), fixed(fb), fixed(down_weight),
         fixed(down_other), fixed((down_bias))],
        [tile_out(width, BF16), tile_out(width, F32), tile_out(width, BF16), tile_out(width, BF16),
         tile_out(width, BF16), tile_out(width, BF16), tile_out(ff, BF16), tile_out(ff, BF16),
         vec_out(width), vec_out(width), vec_out(width), vec_out(width), vec_out(width),
         vec_out(ff), vec_out(ff), vec_out(ff), vec_out(width)],
        [pltpu.VMEM((TILE, ff), F32), pltpu.VMEM((TILE, ff), F32)],
        2 * mm * (width + 2 * ff),
        "middle",
    )

    def merged(left, right, left_side):
        size = (left if left_side else right).shape[1] // 2

        def product(start):
            a = left[:, start : start + size] if left_side else left
            b = right if left_side else right[:, start : start + size]
            return tn(a, b)

        return (product(0) + trade(product(size).astype(BF16)).astype(F32)).astype(BF16)

    down_grad = merged(sub2, cot, True)
    up_grad = merged(normed2, dhid, False)
    out_grad = merged(sub1, dmidb, True)
    dq, dk, dv, g_bq, g_bk, g_bv = call(
        attend_back_kernel,
        pairs,
        [columns(q), columns(k), columns(v), columns(dmix),
         (lse, (1, 8, length), lambda i: (i, 0, 0)), fixed(scol), fixed(srow), fixed(cos), fixed(sin)],
        [pair_out(BF16)] * 3 + [((1, width), F32, (1, PAIR), lambda i: (0, i))] * 3,
        [pltpu.VMEM((spans, TILE), F32), pltpu.VMEM((length, PAIR), F32),
         pltpu.VMEM((length, PAIR), F32)],
        20 * mm * spans // tiles,
        "attend_back",
    )
    qkv_grad = [merged(normed1, d, False) for d in (dq, dk, dv)]
    input_grad, g_ag, g_ab = call(
        finish_kernel,
        tiles,
        [tiled(x, TILE), tiled(dmid, TILE), tiled(dq, TILE), tiled(dk, TILE), tiled(dv, TILE),
         fixed((attn_norm_gain)), fixed(qkv_weight), fixed(qkv_other)],
        [tile_out(width, F32), vec_out(width), vec_out(width)],
        [],
        3 * mm * width,
        "finish",
    )
    cut = [g_bq, g_bk, g_bv, g_sg, g_sb, g_ub, g_fg, g_fb]
    shared = [g_ag, g_ab, g_ob, g_ng, g_nb, g_db]
    mine = jnp.concatenate([c[0, : c.shape[1] // 2] for c in cut] + [s[0] for s in shared])
    theirs = jnp.concatenate([c[0, c.shape[1] // 2 :] for c in cut] + [s[0] for s in shared])
    small = mine + trade(theirs)
    pad = jnp.zeros((-small.size % (16 * PAIR * count),), F32)
    small = jnp.concatenate([small, pad]).astype(BF16).reshape(count, -1, PAIR)
    out_grad = jnp.concatenate([out_grad[:, :half], out_grad[:, half:]])
    blocks = lambda a: a.reshape(count, a.shape[0] // count, a.shape[1])
    plan = []
    for n in range(3):
        for array, stream, size in ((0, 0, width), (1, 1, fhalf)):
            plan.append((array, stream, n * size // 3, (n + 1) * size // 3, n))
        plan.append((2 + n, 2, 0, half, n))
        plan.append((5, 2, n * half // 3, (n + 1) * half // 3, n))
    plan.append((6, 2, 0, PAIR, 2))
    down_grad, up_grad, *qkv_grad, out_grad, small = dp_sum(
        count, [blocks(a) for a in (down_grad, up_grad, *qkv_grad, out_grad)] + [small], plan
    )
    down_grad = down_grad.reshape(fhalf, width)
    up_grad = up_grad.reshape(width, fhalf)
    qkv_grad = jnp.stack([g.reshape(width, half) for g in qkv_grad]).astype(F32)
    out_grad = out_grad.reshape(width, half)
    out_grad = jnp.concatenate([out_grad[:half], out_grad[half:]], axis=1).astype(F32)
    small = small.reshape(-1).astype(F32)
    pieces = []
    at = 0
    for size in [c.shape[1] // 2 for c in cut] + [s.shape[1] for s in shared]:
        pieces.append(small[at : at + size])
        at += size
    g_bq, g_bk, g_bv, g_sg, g_sb, g_ub, g_fg, g_fb, g_ag, g_ab, g_ob, g_ng, g_nb, g_db = pieces
    return (
        outputs[None], input_grad[None], g_ag, g_ab, qkv_grad, jnp.stack([g_bq, g_bk, g_bv]),
        g_sg, g_sb, out_grad, g_ob, g_ng, g_nb, up_grad.astype(F32), g_ub, g_fg, g_fb,
        down_grad.astype(F32), g_db,
    )


def solution(mesh):
    rows = P(("dp", "tensor"), None, None)
    in_specs = (
        rows, P("dp", None), rows, P(), P(), P(None, None, "tensor"), P(None, "tensor"),
        P("tensor"), P("tensor"), P("tensor", None), P(), P(), P(), P(None, "tensor"),
        P("tensor"), P("tensor"), P("tensor"), P("tensor", None), P(),
    )
    out_specs = (
        rows, rows, P(), P(), P(None, None, "tensor"), P(None, "tensor"), P("tensor"), P("tensor"),
        P("tensor", None), P(), P(), P(), P(None, "tensor"), P("tensor"), P("tensor"), P("tensor"),
        P("tensor", None), P(),
    )
    body = functools.partial(local, mesh.shape["dp"])
    return jax.shard_map(body, mesh=mesh, in_specs=in_specs, out_specs=out_specs, check_vma=False)
```
